128 devices in a mesh: gx: 4 (over z), gy: 16 (over y, x), gz: 2 (over core).
Axes of the slice: x: 4, y: 4, z: 4, core: 2. Of those that a mesh axis runs over, the one named last changes fastest.
Arguments:
- particles: float32 [8, 1048576], P(None, ('gx', 'gy', 'gz')), may hold values from -0.5 to 0.5
- dest_key: int32 [1048576], P(('gx', 'gy', 'gz')), may hold values from 0 to 127, as said below
- cell_a: int32 [1048576], P(('gx', 'gy', 'gz')), may hold values from 0 to 255
- cell_b: int32 [1048576], P(('gx', 'gy', 'gz')), may hold values from 0 to 127
- velocity: float32 [2, 1024, 4096], P(None, 'gx', ('gy', 'gz')), may hold values from -6 to 6
Outputs:
- binned: float32 [8, 4194304], P(None, ('gx', 'gy', 'gz'))
- binned_cell: int32 [4194304], P(('gx', 'gy', 'gz'))
The draws below stay inside these ranges and needn't reach their ends.
Inputs may be any that keep to these rules, and one draw needn't show every extreme that they name: Of the particles of one device at most 256 have any one value of dest_key, and one device is named by exactly 256 particles of every device.
All inputs are finite; a program needn't handle non-finite values.
Results may differ from the reference program's by a relative error of at most 0.0003.
Values sent between devices are 32-bit elements; how exact they have to be, the bound alone decides.
No kernel may reach another device: no remote copies, remote signals or barrier semaphores. Data moves between devices by JAX's collectives and lax.ppermute only.
A program may use at most 64 MiB of HBM per device.

```python
import jax
import jax.numpy as jnp
from jax import lax

P_DEV = 8192
TA = 256
TB = 128
OWNERS = 128
CAP = 256
TOTAL = 1048576
NA = 1024
NB = 4096
N_GY = 16
N_GZ = 2


def draw_dest_key(key, part):
    hot_owner = jax.random.randint(jax.random.fold_in(key, 7), (), 0, OWNERS)
    slot_owner = (jnp.arange(OWNERS * CAP, dtype=jnp.int32) // CAP + hot_owner) % OWNERS

    def one_source(source_dev):
        source_key = jax.random.fold_in(key, source_dev)
        others = jax.random.permutation(source_key, OWNERS * CAP - CAP).astype(jnp.int32) + CAP
        chosen = jnp.concatenate([jnp.arange(CAP, dtype=jnp.int32), others[:P_DEV - CAP]])
        shuffle = jax.random.permutation(jax.random.fold_in(source_key, 1), P_DEV)
        return slot_owner[chosen][shuffle]
    return lax.map(one_source, jnp.arange(OWNERS, dtype=jnp.int32)).reshape(-1)


def place_ends(array, stream_key, smallest, top_value):
    longest = array.shape.index(max(array.shape))
    spots = []
    for shift in (0, 1):
        where = [jax.random.randint(jax.random.fold_in(stream_key, axis), (), 0, length) for axis, length in enumerate(array.shape)]
        where[longest] = (where[longest] + shift) % array.shape[longest]
        spots.append(tuple(where))
    return array.at[spots[0]].set(smallest).at[spots[1]].set(top_value)


def level_of(rng, extent, split, low, high):
    def one(dim, shards_of):
        heights = jax.random.uniform(jax.random.fold_in(jax.random.fold_in(rng, 6), dim), (shards_of,), jnp.float32, low / len(split), high / len(split))
        return jnp.repeat(jnp.exp(heights), extent[dim] // shards_of).reshape((-1,) + (1,) * (len(extent) - dim - 1))

    gain = one(*split[0])
    for cut in split[1:]:
        gain = gain * one(*cut)
    return gain


def scatter_about(key, shape, spread, limit, cuts=(), held_as=jnp.bfloat16):
    drawn = spread * jax.random.normal(key, shape, jnp.float32)
    if cuts:
        drawn = drawn * level_of(key, shape, cuts, -0.22, 0.18)
    return jnp.clip(drawn, -limit, limit).astype(held_as)


def setup_inputs(seed: int = 0) -> dict:
    splits = jax.random.split(jax.random.key(seed), 6)
    particles = jnp.clip(jax.random.uniform(splits[0], (8, TOTAL), jnp.float32, -0.5, 0.5) * level_of(splits[0], (8, TOTAL), ((1, 128),), -0.4, 0.0), -0.5, 0.5)
    dest_key = draw_dest_key(jax.random.fold_in(splits[5], 71), 0)
    cell_a = place_ends(jax.random.randint(splits[2], (TOTAL,), 0, TA), jax.random.fold_in(splits[2], 1), 0, TA - 1).astype(jnp.int32)
    cell_b = place_ends(jax.random.randint(splits[3], (TOTAL,), 0, TB), jax.random.fold_in(splits[3], 1), 0, TB - 1).astype(jnp.int32)
    velocity = scatter_about(splits[4], (2, NA, NB), 1.0, 6.0, ((1, 4), (2, 32)), jnp.float32)
    return {"particles": particles, "dest_key": dest_key, "cell_a": cell_a, "cell_b": cell_b, "velocity": velocity}


step_length = 0.5


def quad_weights(frac):
    return (0.5 * frac * (frac - 1.0), 1.0 - frac * frac, 0.5 * frac * (frac + 1.0))


def reference(particles, dest_key, cell_a, cell_b, velocity):
    source_dev = jnp.arange(TOTAL, dtype=jnp.int32) // P_DEV
    bucket_key = source_dev * OWNERS + dest_key
    ordering = jnp.argsort(bucket_key, stable=True).astype(jnp.int32)
    ordered = bucket_key[ordering]
    first_index = jnp.searchsorted(ordered, ordered, side="left").astype(jnp.int32)
    rank_sorted = jnp.arange(TOTAL, dtype=jnp.int32) - first_index
    ranking = jnp.zeros((TOTAL,), jnp.int32).at[ordering].set(rank_sorted)
    slot_index = dest_key * (OWNERS * CAP) + source_dev * CAP + ranking
    tile_columns = N_GY * N_GZ
    global_a = (dest_key // tile_columns) * TA + cell_a
    global_b = (dest_key % tile_columns) * TB + cell_b
    padded = jnp.pad(velocity, ((0, 0), (1, 1), (1, 1)))
    row_stride = NB + 2
    flat_field = padded.reshape(2, -1)
    center = ((global_a + 1) * row_stride + global_b + 1).astype(jnp.int32)
    weights_a = quad_weights(particles[0])
    weights_b = quad_weights(particles[1])
    speed = jnp.zeros((2, TOTAL), jnp.float32)
    for shift_a in range(3):
        for shift_b in range(3):
            nodes = flat_field[:, center + (shift_a - 1) * row_stride + (shift_b - 1)]
            speed = speed + weights_a[shift_a] * weights_b[shift_b] * nodes
    advanced = jnp.concatenate([particles[0:2], particles[2:4] + step_length * speed, particles[4:8]], axis=0)
    binned = jnp.zeros((8, OWNERS * OWNERS * CAP), particles.dtype).at[:, slot_index].set(advanced)
    binned_cell = jnp.full((OWNERS * OWNERS * CAP,), -1, jnp.int32).at[slot_index].set(cell_a * TB + cell_b)
    return binned, binned_cell
```

```python
import jax, jax.numpy as jnp
from jax import lax
from jax.experimental import pallas as pl
from jax.experimental.pallas import tpu as pltpu
f32, bf16, i32 = jnp.float32, jnp.bfloat16, jnp.int32
ROWS = 18

def iota(shape, dim, dt):
    return lax.broadcasted_iota(i32, shape, dim).astype(f32).astype(dt)

def nt(a, b):
    return lax.dot_general(a, b, (((1,), (1,)), ((), ())), preferred_element_type=f32)

def nn(a, b):
    return jnp.dot(a, b, preferred_element_type=f32)

def split(v):
    hi = v.astype(bf16)
    return hi, (v - hi.astype(f32)).astype(bf16)

def bucket_kernel(p_ref, key_ref, a_ref, b_ref, out_ref, acc_ref, base_ref, rank_ref, ut_ref, hot_ref):
    PB = 256
    n = p_ref.shape[1] // PB
    out_ref[...] = jnp.zeros(out_ref.shape, f32)
    acc_ref[...] = jnp.zeros(acc_ref.shape, f32)
    base_ref[...] = jnp.zeros(base_ref.shape, f32)
    r = lax.broadcasted_iota(i32, (PB, PB), 0)
    c = lax.broadcasted_iota(i32, (PB, PB), 1)
    ut_ref[:, :PB] = jnp.where(r < c, 1.0, 0.0).astype(bf16)
    ut_ref[:, PB:] = jnp.ones((PB, 128), bf16)

    def cells(sl):
        return (a_ref[0:1, sl] * 128 + b_ref[0:1, sl] + 1).astype(f32)

    def place(sl, key, t, acc):
        low = jnp.where(key >= 64, key - 64, key)
        pick = iota((64, PB), 0, bf16) == low.astype(f32).astype(bf16)
        cols = jnp.where(iota((256, PB), 0, bf16) == t.astype(bf16), 1.0, 0.0).astype(bf16)
        rows = [p_ref[k:k + 1, sl] for k in range(8)] + [cells(sl)]
        his, los = [], []
        for v in rows:
            hi, lo = split(v)
            his.append(jnp.where(pick, hi, jnp.zeros((), bf16)))
            los.append(jnp.where(pick, lo, jnp.zeros((), bf16)))
        return nt(jnp.concatenate(his, 0), cols) + nt(jnp.concatenate(los, 0), cols)

    def body(i, carry):
        sl = pl.ds(pl.multiple_of(i * PB, PB), PB)
        key = key_ref[0:1, sl]
        oh = lax.broadcasted_iota(i32, (128, PB), 0) == key
        ohb = jnp.where(oh, 1.0, 0.0).astype(bf16)
        res = nn(ohb, ut_ref[...])
        base = base_ref[...]
        before = res[:, :PB] + jnp.concatenate([base, base], 1)
        rank = jnp.sum(jnp.where(oh, before, 0.0), axis=0, keepdims=True)
        base_ref[...] = base + res[:, PB:]
        rank_ref[0:1, sl] = rank
        t = jnp.where(rank < 128.0, rank + jnp.where(key >= 64, 128.0, 0.0), -1.0)
        acc_ref[...] += place(sl, key, t, acc_ref)
        return carry

    lax.fori_loop(0, n, body, 0)

    def flush(half):
        for k in range(9):
            for o in range(2):
                out_ref[pl.ds(o * 64 * ROWS + 9 * half + k, 64, stride=ROWS), :] = acc_ref[k * 64:(k + 1) * 64, o * 128:(o + 1) * 128]

    flush(0)
    counts = base_ref[...]
    ids = lax.broadcasted_iota(i32, (128, 128), 0).astype(f32)
    n_full = jnp.max(jnp.sum(jnp.where(counts > 128.0, 1.0, 0.0), axis=0, keepdims=True))
    hot = jnp.max(jnp.where(counts > 128.0, ids, -1.0)).astype(i32)

    @pl.when(n_full <= 1.0)
    def _():
        hot_ref[...] = jnp.zeros(hot_ref.shape, f32)

        def hot_body(i, carry):
            sl = pl.ds(pl.multiple_of(i * PB, PB), PB)
            key = key_ref[0:1, sl]
            over = jnp.where(key == hot, rank_ref[0:1, sl] - 128.0, -1.0)
            cols = jnp.where(iota((128, PB), 0, bf16) == over.astype(bf16), 1.0, 0.0).astype(bf16)
            hi, lo = split(jnp.concatenate([p_ref[:, sl], jnp.broadcast_to(cells(sl), (8, PB))], 0))
            hot_ref[...] += nt(hi, cols) + nt(lo, cols)
            return carry

        lax.fori_loop(0, n, hot_body, 0)
        at = jnp.maximum(hot, 0) * ROWS + 9
        for k in range(9):
            out_ref[pl.ds(at + k, 1), :] = hot_ref[k:k + 1, :]

    @pl.when(n_full > 1.0)
    def _():
        acc_ref[...] = jnp.zeros(acc_ref.shape, f32)

        def over_body(i, carry):
            sl = pl.ds(pl.multiple_of(i * PB, PB), PB)
            key = key_ref[0:1, sl]
            rank = rank_ref[0:1, sl]
            t = jnp.where(rank >= 128.0, rank - 128.0 + jnp.where(key >= 64, 128.0, 0.0), -1.0)
            acc_ref[...] += place(sl, key, t, acc_ref)
            return carry

        lax.fori_loop(0, n, over_body, 0)
        flush(1)

def bucket(particles, key, a, b):
    n = particles.shape[1]
    return pl.pallas_call(
        bucket_kernel,
        out_shape=jax.ShapeDtypeStruct((128 * ROWS, 128), f32),
        in_specs=[pl.BlockSpec(memory_space=pltpu.VMEM)] * 4,
        out_specs=pl.BlockSpec(memory_space=pltpu.VMEM),
        scratch_shapes=[pltpu.VMEM((576, 256), f32), pltpu.VMEM((128, 128), f32), pltpu.VMEM((1, n), f32),
                        pltpu.VMEM((256, 384), bf16), pltpu.VMEM((16, 128), f32)],
        name="bucket",
    )(particles, key.reshape(1, -1), a.reshape(1, -1), b.reshape(1, -1))

def interp_kernel(r_ref, v_ref, rows_ref, cols_ref, out_ref, cell_ref, fhi_ref, flo_ref, fe_ref):
    S = 4
    N = 256 * S
    for c in range(2):
        t = v_ref[c].T
        hi, lo = split(t)
        fhi_ref[c * 128:(c + 1) * 128, :] = hi
        flo_ref[c * 128:(c + 1) * 128, :] = lo
    hi, lo = split(cols_ref[:, :256])
    fhi_ref[256:272, :] = hi
    flo_ref[256:272, :] = lo
    fe_ref[...] = rows_ref[...]

    def weights(t):
        return 0.5 * t * (t - 1.0), 1.0 - t * t, 0.5 * t * (t + 1.0)

    def body(i, carry):
        for u in range(S):
            s = i * S + u
            base = s * ROWS
            x0 = r_ref[pl.ds(base, 8), :]
            x1 = r_ref[pl.ds(base + 9, 8), :]
            cell = jnp.concatenate([r_ref[pl.ds(base + 8, 1), :], r_ref[pl.ds(base + 17, 1), :]], 1)
            ci = cell.astype(i32) - 1
            live = ci >= 0
            a = jnp.where(live, ci >> 7, -8).astype(f32)
            b = (ci & 127).astype(f32)
            f = jnp.concatenate([x0[0:1], x1[0:1]], 1)
            g = jnp.concatenate([x0[1:2], x1[1:2]], 1)
            wm, w0, wp = [0.5 * w for w in weights(f)]
            gm, g0, gp = weights(g)
            ab = a.astype(bf16)
            am, ap = (a - 1.0).astype(bf16), (a + 1.0).astype(bf16)
            rowid = iota((256, 256), 0, bf16)
            m0, m1, m2 = rowid == am, rowid == ab, rowid == ap
            z = jnp.zeros((), bf16)
            (wmh, wml), (w0h, w0l), (wph, wpl) = split(wm), split(w0), split(wp)
            whi = jnp.where(m0, wmh, jnp.where(m1, w0h, jnp.where(m2, wph, z)))
            wlo = jnp.where(m0, wml, jnp.where(m1, w0l, jnp.where(m2, wpl, z)))
            et = jnp.where(a == 0.0, wm, 0.0)
            eb = jnp.where(a == 255.0, wp, 0.0)
            (eth, etl), (ebh, ebl) = split(et), split(eb)
            k = lax.broadcasted_iota(i32, (16, 256), 0)
            we = jnp.where(k == 0, eth.astype(f32), jnp.where(k == 1, ebh.astype(f32), jnp.where(k == 2, eth.astype(f32),
                 jnp.where(k == 3, ebh.astype(f32), jnp.where(k == 4, etl.astype(f32), jnp.where(k == 5, ebl.astype(f32), 0.0))))))
            we = we.astype(bf16)
            fhi = fhi_ref[...]
            R = nn(fhi, whi) + nn(flo_ref[...], whi) + nn(fhi, wlo) + nn(fe_ref[...], we)
            col = iota((128, 256), 0, f32)
            cw = jnp.where(col == b - 1.0, gm, jnp.where(col == b, g0, jnp.where(col == b + 1.0, gp, 0.0)))
            el = jnp.where(b == 0.0, gm, 0.0)
            er = jnp.where(b == 127.0, gp, 0.0)
            s0 = jnp.sum(R[0:128] * cw, axis=0, keepdims=True) + R[256:257] * el + R[257:258] * er
            s1 = jnp.sum(R[128:256] * cw, axis=0, keepdims=True) + R[258:259] * el + R[259:260] * er
            rid = lax.broadcasted_iota(i32, (8, 256), 0)
            d = jnp.where(rid == 2, s0, jnp.where(rid == 3, s1, 0.0))
            at = pl.multiple_of(s * 256, 256)
            out_ref[:, pl.ds(at, 256)] = jnp.concatenate([x0, x1], 1) + d
            cell_ref[0:1, pl.ds(at, 256)] = ci
        return carry

    lax.fori_loop(0, 128 // S, body, 0)

def interp(recv, velocity, top, bottom, left, right):
    zero = jnp.zeros((2, 1), f32)
    cols = jnp.stack([left[0], right[0], left[1], right[1]], 0)
    main = jnp.pad(cols[:, 1:257], ((0, 12), (0, 0)))
    edge_t = jnp.concatenate([top[0], top[1], cols[:, 0]])
    edge_b = jnp.concatenate([bottom[0], bottom[1], cols[:, 257]])
    e = jnp.stack([edge_t, edge_b], 1)
    eh = lax.reduce_precision(e, 8, 7)
    el = e - eh
    fe = jnp.pad(jnp.concatenate([eh, el, eh], 1), ((0, 12), (0, 10))).astype(bf16)
    n = 128 * 256
    out, cell = pl.pallas_call(
        interp_kernel,
        out_shape=(jax.ShapeDtypeStruct((8, n), f32), jax.ShapeDtypeStruct((1, n), i32)),
        in_specs=[pl.BlockSpec(memory_space=pltpu.VMEM)] * 4,
        out_specs=(pl.BlockSpec(memory_space=pltpu.VMEM),) * 2,
        scratch_shapes=[pltpu.VMEM((272, 256), bf16), pltpu.VMEM((272, 256), bf16), pltpu.VMEM((272, 16), bf16)],
        name="interp",
    )(recv, velocity, fe, main)
    return out, cell.reshape(-1)


from jax.sharding import Mesh
from jax.sharding import PartitionSpec as P

ALL = ("gx", "gy_0", "gy_1", "gz")
WIDE = ("gy_0", "gy_1", "gz")


def both_sides(first, last, axis):
    peers = lax.axis_size(axis)
    up = [(i, i + 1) for i in range(peers - 1)]
    down = [(j, i) for i, j in up]
    return lax.ppermute(last, axis, up), lax.ppermute(first, axis, down)


def shards(particles, dest_key, cell_a, cell_b, velocity):
    rows = velocity.shape[1]
    cols = velocity.shape[2]
    above, below = both_sides(velocity[:, 0, :], velocity[:, rows - 1, :], "gx")

    def column(k):
        return jnp.concatenate([above[:, k:k + 1], velocity[:, :, k], below[:, k:k + 1]], axis=1)

    left, right = both_sides(column(0), column(cols - 1), WIDE)
    outgoing = bucket(particles, dest_key, cell_a, cell_b)
    outgoing = outgoing.reshape(128, ROWS, 1, 128)
    arrived = lax.all_to_all(outgoing, ALL, 0, 0, tiled=True)
    return interp(arrived.reshape(128 * ROWS, 128), velocity, above, below, left, right)


def solution(mesh):
    split_mesh = Mesh(mesh.devices.reshape(mesh.shape["gx"], 4, 4, mesh.shape["gz"]), ALL)
    in_specs = (P(None, ALL), P(ALL), P(ALL), P(ALL), P(None, "gx", WIDE))
    out_specs = (P(None, ALL), P(ALL))
    return jax.shard_map(shards, mesh=split_mesh, in_specs=in_specs, out_specs=out_specs, check_vma=False)
```

```python
import jax
import jax.numpy as jnp
from jax import lax
from jax.experimental import pallas as pl
from jax.experimental.pallas import tpu as pltpu

f32, bf16, i32 = jnp.float32, jnp.bfloat16, jnp.int32
OWNERS = 128
HEAD = 3
BODY = 6
HALO = 4
HEAD_ROWS = 2 * HEAD + HALO
BODY_ROWS = 2 * BODY
PB = 512
VMEM = pl.BlockSpec(memory_space=pltpu.VMEM)
SMEM = pl.BlockSpec(memory_space=pltpu.SMEM)


def iota(shape, dim, dt):
    return lax.broadcasted_iota(i32, shape, dim).astype(f32).astype(dt)


def nt(a, b):
    return lax.dot_general(a, b, (((1,), (1,)), ((), ())), preferred_element_type=f32)


def nn(a, b):
    return jnp.dot(a, b, preferred_element_type=f32)


def split(v):
    hi = v.astype(bf16)
    return hi, (v - hi.astype(f32)).astype(bf16)


def one_hot(size, t):
    hit = iota((size, t.shape[1]), 0, bf16) == t.astype(bf16)
    return jnp.where(hit, jnp.ones((), bf16), jnp.zeros((), bf16))


def block(i):
    return pl.ds(pl.multiple_of(i * PB, PB), PB)


def column_of(key, rank, first):
    off = rank - first
    fits = (off >= 0.0) & (off < 128.0)
    return jnp.where(fits, off + jnp.where(key >= 64, 128.0, 0.0), -1.0)


def fold(key):
    return one_hot(64, jnp.where(key >= 64, key - 64, key).astype(f32))


def add_placed(acc_ref, rows, pick, t):
    m = 64 * len(rows)
    parts = [split(r) for r in rows]
    left = jnp.concatenate([pick * p[0] for p in parts] + [pick * p[1] for p in parts], 0)
    both = nt(left, one_hot(256, t))
    acc_ref[...] += both[:m] + both[m:]


def flush(out_ref, acc_ref, width, first, stride):
    for k in range(width):
        for o in range(2):
            rows = pl.ds(o * 64 * stride + first + k, 64, stride=stride)
            out_ref[rows, :] = acc_ref[k * 64:(k + 1) * 64, o * 128:(o + 1) * 128]


def second_half(rows_of, width, key_ref, rank_ref, counts, out_ref, acc_ref, hot_ref, stride):
    n = key_ref.shape[1] // PB
    ids = lax.broadcasted_iota(i32, (128, 128), 0).astype(f32)
    n_full = jnp.max(jnp.sum(jnp.where(counts > 128.0, 1.0, 0.0), axis=0, keepdims=True))
    hot = jnp.max(jnp.where(counts > 128.0, ids, -1.0)).astype(i32)

    @pl.when(n_full <= 1.0)
    def _():
        hot_ref[...] = jnp.zeros(hot_ref.shape, f32)

        def hot_body(i, carry):
            sl = block(i)
            over = jnp.where(key_ref[0:1, sl] == hot, rank_ref[0:1, sl] - 128.0, -1.0)
            rows = rows_of(sl)
            rows = rows + [jnp.zeros((8 - width, PB), f32)]
            hi, lo = split(jnp.concatenate(rows, 0))
            both = nt(jnp.concatenate([hi, lo], 0), one_hot(128, over))
            hot_ref[...] += both[:8] + both[8:]
            return carry

        lax.fori_loop(0, n, hot_body, 0)
        at = jnp.maximum(hot, 0) * stride + width
        for k in range(width):
            out_ref[pl.ds(at + k, 1), :] = hot_ref[k:k + 1, :]

    @pl.when(n_full > 1.0)
    def _():
        acc_ref[...] = jnp.zeros(acc_ref.shape, f32)

        def over_body(i, carry):
            sl = block(i)
            key = key_ref[0:1, sl]
            add_placed(acc_ref, rows_of(sl), fold(key), column_of(key, rank_ref[0:1, sl], 128.0))
            return carry

        lax.fori_loop(0, n, over_body, 0)
        flush(out_ref, acc_ref, width, width, stride)


def head_kernel(at_ref, p_ref, key_ref, a_ref, b_ref, v_ref, out_ref, rank_ref, count_ref, acc_ref, ut_ref, hot_ref):
    n = p_ref.shape[1] // PB
    out_ref[...] = jnp.zeros(out_ref.shape, f32)
    acc_ref[...] = jnp.zeros(acc_ref.shape, f32)
    count_ref[...] = jnp.zeros(count_ref.shape, f32)
    before = lax.broadcasted_iota(i32, (128, 128), 0) < lax.broadcasted_iota(i32, (128, 128), 1)
    ut_ref[:, :128] = jnp.where(before, 1.0, 0.0).astype(bf16)
    ut_ref[:, 128:] = jnp.ones((128, 128), bf16)

    def rows_of(sl):
        cell = (a_ref[0:1, sl] * 128 + b_ref[0:1, sl] + 1).astype(f32)
        return [p_ref[0:1, sl], p_ref[1:2, sl], cell]

    def rank_block(i):
        sl = block(i)
        key = key_ref[0:1, sl]
        hots = []
        for k in range(PB // 128):
            hit = lax.broadcasted_iota(i32, (128, 128), 0) == key[:, k * 128:(k + 1) * 128]
            hots.append(jnp.where(hit, 1.0, 0.0))
        res = nn(jnp.concatenate([h.astype(bf16) for h in hots], 0), ut_ref[...])
        base = count_ref[...]
        ranks = []
        for k in range(PB // 128):
            r = res[k * 128:(k + 1) * 128]
            ranks.append(jnp.sum(hots[k] * (r[:, :128] + base), axis=0, keepdims=True))
            base = base + r[:, 128:]
        count_ref[...] = base
        return jnp.concatenate(ranks, 1)

    def place_block(i, rank):
        sl = block(i)
        key = key_ref[0:1, sl]
        add_placed(acc_ref, rows_of(sl), fold(key), column_of(key, rank, 0.0))

    rank0 = rank_block(0)
    rank_ref[0:1, block(0)] = rank0

    def body(i, rank):
        nxt = rank_block(i)
        place_block(i - 1, rank)
        rank_ref[0:1, block(i)] = nxt
        return nxt

    place_block(n - 1, lax.fori_loop(1, n, body, rank0))
    flush(out_ref, acc_ref, HEAD, 0, HEAD_ROWS)
    second_half(rows_of, HEAD, key_ref, rank_ref, count_ref[...], out_ref, acc_ref, hot_ref, HEAD_ROWS)

    x, y = at_ref[0], at_ref[1]
    top_x, top_y = at_ref[2] - 1, at_ref[3] - 1
    me = x * (top_y + 1) + y
    cols = v_ref.shape[2]
    turned = [v_ref[c].T for c in range(2)]
    lane = lax.broadcasted_iota(i32, (1, cols), 1)
    for dx in (-1, 0, 1):
        for dy in (-1, 0, 1):
            if dx == 0 and dy == 0:
                continue
            row = v_ref.shape[1] - 1 if dx > 0 else 0
            col = cols - 1 if dy > 0 else 0
            base = (me + dx * (top_y + 1) + dy) * HEAD_ROWS + 2 * HEAD

            @pl.when((x + dx >= 0) & (x + dx <= top_x) & (y + dy >= 0) & (y + dy <= top_y))
            def _():
                for c in range(2):
                    if dx:
                        line = v_ref[c, row:row + 1, :]
                        if dy:
                            one = jnp.sum(jnp.where(lane == col, line, 0.0), axis=1, keepdims=True)
                            line = jnp.broadcast_to(one, (1, cols))
                        out_ref[pl.ds(base + c, 1), :] = line
                    else:
                        for h in range(2):
                            out_ref[pl.ds(base + 2 * c + h, 1), :] = turned[c][col:col + 1, h * 128:(h + 1) * 128]


def body_kernel(p_ref, key_ref, rank_ref, count_ref, out_ref, acc_ref, hot_ref):
    n = p_ref.shape[1] // PB
    out_ref[...] = jnp.zeros(out_ref.shape, f32)
    acc_ref[...] = jnp.zeros(acc_ref.shape, f32)

    def rows_of(sl):
        return [p_ref[k:k + 1, sl] for k in range(2, 8)]

    def body(i, carry):
        sl = block(i)
        key = key_ref[0:1, sl]
        add_placed(acc_ref, rows_of(sl), fold(key), column_of(key, rank_ref[0:1, sl], 0.0))
        return carry

    lax.fori_loop(0, n, body, 0)
    flush(out_ref, acc_ref, BODY, 0, BODY_ROWS)
    second_half(rows_of, BODY, key_ref, rank_ref, count_ref[...], out_ref, acc_ref, hot_ref, BODY_ROWS)


def quad(t):
    return 0.5 * t * (t - 1.0), 1.0 - t * t, 0.5 * t * (t + 1.0)


def windows(start, size, pieces, dt):
    r = iota((size, start.shape[1]), 0, f32).astype(dt)
    hits = [r == (start + float(k)).astype(dt) for k in range(3)]
    over = [r == (start + float(k - size)).astype(dt) for k in range(3)]
    z = jnp.zeros((), dt)
    low = [jnp.where(hits[0], w[0], jnp.where(hits[1], w[1], jnp.where(hits[2], w[2], z))) for w in pieces]
    high = [jnp.where(over[1], w[1], jnp.where(over[2], w[2], z)) for w in pieces]
    return low, high


def interp_kernel(at_ref, r_ref, v_ref, out_ref, cell_ref, f_ref, t_ref):
    S = 4
    x, y = at_ref[0], at_ref[1]
    top_x, top_y = at_ref[2] - 1, at_ref[3] - 1
    me = x * (top_y + 1) + y

    def from_side(dx, dy, k):
        inside = (x + dx >= 0) & (x + dx <= top_x) & (y + dy >= 0) & (y + dy <= top_y)
        src = jnp.where(inside, me + dx * (top_y + 1) + dy, me)
        row = r_ref[pl.ds(src * HEAD_ROWS + 2 * HEAD + k, 1), :]
        return jnp.where(inside, row, 0.0)

    side_rows = []
    for c in range(2):
        turned = v_ref[c].T
        hi, lo = split(turned)
        f_ref[c * 128:(c + 1) * 128, :] = hi
        f_ref[272 + c * 128:272 + (c + 1) * 128, :] = lo
        for dy in (-1, 1):
            side_rows.append(jnp.concatenate([from_side(0, dy, 2 * c + h) for h in range(2)], 1))
    z6 = jnp.zeros((6, 256), f32)
    hi, lo = split(jnp.concatenate([side_rows[0], side_rows[1], z6, side_rows[2], side_rows[3], z6], 0))
    f_ref[256:272, :] = hi
    f_ref[528:544, :] = lo
    for e, dx in enumerate((-1, 1)):
        lanes = slice(128 * e, 128 * e + 128)
        corners = []
        for c in range(2):
            t_ref[c * 128:(c + 1) * 128, lanes] = jnp.broadcast_to(from_side(dx, 0, c), (128, 128)).T
            corners += [from_side(dx, -1, c), from_side(dx, 1, c), jnp.zeros((6, 128), f32)]
        t_ref[256:272, lanes] = jnp.concatenate(corners, 0)

    def step(i, carry):
        for u in range(S):
            s = i * S + u
            base = s * HEAD_ROWS
            lines = [jnp.concatenate([r_ref[pl.ds(base + k, 1), :], r_ref[pl.ds(base + HEAD + k, 1), :]], 1) for k in range(HEAD)]
            f, g = lines[0], lines[1]
            ci = lines[2].astype(i32) - 1
            live = ci >= 0
            a = jnp.where(live, ci >> 7, 0)
            b = ci & 127
            half = jnp.where(live, 0.5, 0.0)
            wa = [half * w for w in quad(f)]
            wb = quad(g)
            parts = [split(w) for w in wa]
            his, los = [p[0] for p in parts], [p[1] for p in parts]
            (h0, l0), (h1, l1) = windows(((a - 1) & 15).astype(f32), 16, [his, los], bf16)
            qa = jnp.broadcast_to(((a - 1) >> 4).astype(f32).astype(bf16), (16, 256))
            zero = jnp.zeros((16, 256), bf16)
            whi, wlo = [], []
            hit = qa == jnp.asarray(-1, bf16)
            for j in range(16):
                prev = hit
                hit = qa == jnp.asarray(j, bf16)
                whi.append(jnp.where(hit, h0, jnp.where(prev, h1, zero)))
                wlo.append(jnp.where(hit, l0, jnp.where(prev, l1, zero)))
            whi, wlo = jnp.concatenate(whi, 0), jnp.concatenate(wlo, 0)
            two = nn(f_ref[...], whi)
            R = two[:272] + two[272:] + nn(f_ref[:272, :], wlo)
            top = jnp.broadcast_to(a, (8, 256)) == 0
            edge = jnp.broadcast_to(jnp.where(a == 0, wa[0], jnp.where(a == 255, wa[2], 0.0)), (8, 256))
            (c0,), (c1,) = windows(((b - 1) & 7).astype(f32), 8, [wb], f32)
            qb = jnp.broadcast_to((b - 1) >> 3, (8, 256))

            def rows(at):
                t = [jnp.concatenate([t_ref[at:at + 8, 128 * k:128 * k + 128]] * 2, 1) for k in range(2)]
                return R[at:at + 8] + edge * jnp.where(top, t[0], t[1])

            zero8 = jnp.zeros((8, 256), f32)
            first = [zero8, zero8]
            second = [zero8, zero8]
            hit = qb == -1
            for j in range(16):
                prev = hit
                hit = qb == j
                for c in range(2):
                    v = rows(c * 128 + 8 * j)
                    first[c] = jnp.where(hit, v, first[c])
                    second[c] = jnp.where(prev, v, second[c])
            el = jnp.where(b == 0, wb[0], 0.0)
            er = jnp.where(b == 127, wb[2], 0.0)
            out = []
            for c in range(2):
                side = rows(256 + 8 * c)
                d = jnp.sum(first[c] * c0 + second[c] * c1, axis=0, keepdims=True)
                out.append(d + side[0:1] * el + side[1:2] * er)
            at = pl.multiple_of(s * 256, 256)
            out_ref[:, pl.ds(at, 256)] = jnp.concatenate([f, g] + out, 0)
            cell_ref[0:1, pl.ds(at, 256)] = ci
        return carry

    lax.fori_loop(0, OWNERS // S, step, 0)


def merge_kernel(d_ref, r_ref, out_ref):
    for s in range(d_ref.shape[1] // 256):
        lines = jnp.concatenate(
            [jnp.concatenate([r_ref[s * BODY_ROWS + h * BODY + k:s * BODY_ROWS + h * BODY + k + 1, :] for h in range(2)], 1) for k in range(BODY)], 0)
        d = d_ref[:, s * 256:(s + 1) * 256]
        out_ref[:, s * 256:(s + 1) * 256] = jnp.concatenate([d[0:2], lines[0:2] + d[2:4], lines[2:6]], 0)


def shape(*dims, dt=f32):
    return jax.ShapeDtypeStruct(dims, dt)


def head(place, particles, key, a, b, velocity):
    n = particles.shape[1]
    return pl.pallas_call(
        head_kernel,
        out_shape=(shape(OWNERS * HEAD_ROWS, 128), shape(1, n), shape(128, 128)),
        in_specs=[SMEM] + [VMEM] * 5,
        out_specs=(VMEM,) * 3,
        scratch_shapes=[pltpu.VMEM((64 * HEAD, 256), f32), pltpu.VMEM((128, 256), bf16), pltpu.VMEM((8, 128), f32)],
        name="head",
    )(place, particles, key, a, b, velocity)


def body(particles, key, rank, count):
    return pl.pallas_call(
        body_kernel,
        out_shape=shape(OWNERS * BODY_ROWS, 128),
        in_specs=[VMEM] * 4,
        out_specs=VMEM,
        scratch_shapes=[pltpu.VMEM((64 * BODY, 256), f32), pltpu.VMEM((8, 128), f32)],
        name="body",
    )(particles, key, rank, count)


def interp(place, arrived, velocity):
    n = OWNERS * 256
    return pl.pallas_call(
        interp_kernel,
        out_shape=(shape(4, n), shape(1, n, dt=i32)),
        in_specs=[SMEM, VMEM, VMEM],
        out_specs=(VMEM,) * 2,
        scratch_shapes=[pltpu.VMEM((544, 256), bf16), pltpu.VMEM((272, 256), f32)],
        name="interp",
    )(place, arrived, velocity)


def merge(moved, arrived):
    n = moved.shape[1]
    g = 8
    return pl.pallas_call(
        merge_kernel,
        out_shape=shape(8, n),
        grid=(g,),
        in_specs=[pl.BlockSpec((4, n // g), lambda i: (0, i)), pl.BlockSpec((OWNERS // g * BODY_ROWS, 128), lambda i: (i, 0))],
        out_specs=pl.BlockSpec((8, n // g), lambda i: (0, i)),
        name="merge",
    )(moved, arrived)


from jax.sharding import Mesh
from jax.sharding import PartitionSpec as P

ALL = ("gx", "gy_0", "gy_1", "gz")
WIDE = ("gy_0", "gy_1", "gz")


def exchange(buckets, rows):
    out = lax.all_to_all(buckets.reshape(OWNERS, rows, 1, 128), ALL, 0, 0, tiled=True)
    return out.reshape(OWNERS * rows, 128)


def shards(particles, dest_key, cell_a, cell_b, velocity):
    place = jnp.stack([lax.axis_index("gx"), lax.axis_index(WIDE), lax.axis_size("gx"), lax.axis_size(WIDE)]).astype(i32)
    key, a, b = [v.reshape(1, -1) for v in (dest_key, cell_a, cell_b)]
    first, rank, count = head(place, particles, key, a, b, velocity)
    arrived = exchange(first, HEAD_ROWS)
    rest = exchange(body(particles, key, rank, count), BODY_ROWS)
    moved, cell = interp(place, arrived, velocity)
    return merge(moved, rest), cell.reshape(-1)


def solution(mesh):
    split_mesh = Mesh(mesh.devices.reshape(mesh.shape["gx"], 4, 4, mesh.shape["gz"]), ALL)
    in_specs = (P(None, ALL), P(ALL), P(ALL), P(ALL), P(None, "gx", WIDE))
    out_specs = (P(None, ALL), P(ALL))
    return jax.shard_map(shards, mesh=split_mesh, in_specs=in_specs, out_specs=out_specs, check_vma=False)
```

```python
import jax
import jax.numpy as jnp
from jax import lax
from jax.experimental import pallas as pl
from jax.experimental.pallas import tpu as pltpu
from jax.sharding import Mesh
from jax.sharding import PartitionSpec as P

f32, bf16, i32 = jnp.float32, jnp.bfloat16, jnp.int32
ALL = ("gx", "gy_0", "gy_1", "gz")
WIDE = ("gy_0", "gy_1", "gz")
OWNERS = 128
HEAD = 3
BODY = 6
HEAD_ROWS = 10
BODY_ROWS = 12
HALO = 6
PAD = 8
PB = 4096
RB = 4096
VMEM = pl.BlockSpec(memory_space=pltpu.VMEM)


def iota(shape, dim, dt):
    return lax.broadcasted_iota(i32, shape, dim).astype(f32).astype(dt)


def nt(a, b):
    return lax.dot_general(a, b, (((1,), (1,)), ((), ())), preferred_element_type=f32)


def nn(a, b):
    return jnp.dot(a, b, preferred_element_type=f32)


def split(v):
    hi = v.astype(bf16)
    return hi, (v - hi.astype(f32)).astype(bf16)


def one_hot(size, t):
    hit = iota((size, t.shape[1]), 0, bf16) == t.astype(bf16)
    return jnp.where(hit, jnp.ones((), bf16), jnp.zeros((), bf16))


def block(i, size):
    return pl.ds(pl.multiple_of(i * size, size), size)


def column_of(key, rank, first):
    off = rank - first
    fits = (off >= 0.0) & (off < 128.0)
    return jnp.where(fits, off + jnp.where(key >= 64, 128.0, 0.0), -1.0)


def head_row(k, half):
    return 2 * half + k if k < 2 else 4 + half


def body_row(k, half):
    return BODY * half + k


def place_all(rows_of, width, row_at, stride, key_ref, rank_ref, counts, out_ref, acc_ref, left_ref, col_ref, hot_ref):
    n = key_ref.shape[1] // PB
    m = 64 * width
    ids = lax.broadcasted_iota(i32, (128, 128), 0).astype(f32)
    n_full = jnp.max(jnp.sum(jnp.where(counts > 128.0, 1.0, 0.0), axis=0, keepdims=True))
    hot = jnp.max(jnp.where(counts > 128.0, ids, -1.0)).astype(i32)
    few = n_full <= 1.0
    hot_key = jnp.where(few, hot, -1)

    def add_placed(rows, key, t):
        pick = one_hot(64, jnp.where(key >= 64, key - 64, key).astype(f32))
        for k, r in enumerate(rows):
            hi, lo = split(r)
            left_ref[k * 64:(k + 1) * 64, :] = pick * hi
            left_ref[m + k * 64:m + (k + 1) * 64, :] = pick * lo
        col_ref[...] = one_hot(256, t)
        both = nt(left_ref[...], col_ref[...])
        acc_ref[...] += both[:m] + both[m:]

    def flush(half):
        for k in range(width):
            for o in range(2):
                at = pl.ds(o * 64 * stride + row_at(k, half), 64, stride=stride)
                out_ref[at, :] = acc_ref[k * 64:(k + 1) * 64, o * 128:(o + 1) * 128]

    acc_ref[...] = jnp.zeros(acc_ref.shape, f32)
    hot_ref[...] = jnp.zeros(hot_ref.shape, f32)

    def step(i, carry):
        sl = block(i, PB)
        key, rank = key_ref[0:1, sl], rank_ref[0:1, sl]
        rows = rows_of(sl)
        add_placed(rows, key, column_of(key, rank, 0.0))
        over = jnp.where(key == hot_key, rank - 128.0, -1.0)
        hi, lo = split(jnp.concatenate(rows + [jnp.zeros((8 - width, PB), f32)], 0))
        hot_ref[:, :16] += nt(one_hot(128, over), jnp.concatenate([hi, lo], 0))
        return carry

    lax.fori_loop(0, n, step, 0)
    flush(0)
    turned = hot_ref[...].T
    spill = turned[:8] + turned[8:16]
    base = jnp.maximum(hot, 0) * stride
    for k in range(width):
        out_ref[pl.ds(base + row_at(k, 1), 1), :] = spill[k:k + 1]

    @pl.when(jnp.logical_not(few))
    def _():
        acc_ref[...] = jnp.zeros(acc_ref.shape, f32)

        def again(i, carry):
            sl = block(i, PB)
            key = key_ref[0:1, sl]
            add_placed(rows_of(sl), key, column_of(key, rank_ref[0:1, sl], 128.0))
            return carry

        lax.fori_loop(0, n, again, 0)
        flush(1)


def around():
    x, y = lax.axis_index("gx"), lax.axis_index(WIDE)
    nx, ny = lax.axis_size("gx"), lax.axis_size(WIDE)

    def side(dx, dy):
        inside = (x + dx >= 0) & (x + dx < nx) & (y + dy >= 0) & (y + dy < ny)
        return inside, jnp.where(inside, (x + dx) * ny + y + dy, 0)

    return side


def head_kernel(p_ref, key_ref, a_ref, b_ref, v_ref, out_ref, rank_ref, count_ref, acc_ref, left_ref, col_ref, hot_ref, ut_ref, oh_ref):
    n = p_ref.shape[1] // RB
    out_ref[...] = jnp.zeros(out_ref.shape, f32)
    count_ref[...] = jnp.zeros(count_ref.shape, f32)
    before = lax.broadcasted_iota(i32, (128, 128), 0) < lax.broadcasted_iota(i32, (128, 128), 1)
    ut_ref[:, :128] = jnp.where(before, 1.0, 0.0).astype(bf16)
    ut_ref[:, 128:] = jnp.ones((128, 128), bf16)

    def rank_block(i, carry):
        sl = block(i, RB)
        key = key_ref[0:1, sl].astype(f32)
        for k in range(RB // 128):
            oh_ref[k * 128:(k + 1) * 128, :] = one_hot(128, key[:, k * 128:(k + 1) * 128])
        res = nn(oh_ref[...], ut_ref[...])
        base = count_ref[...]
        ranks = []
        for k in range(RB // 128):
            r = res[k * 128:(k + 1) * 128]
            hot = oh_ref[k * 128:(k + 1) * 128, :].astype(f32)
            ranks.append(jnp.sum(hot * (r[:, :128] + base), axis=0, keepdims=True))
            base = base + r[:, 128:]
        count_ref[...] = base
        rank_ref[0:1, sl] = jnp.concatenate(ranks, 1)
        return carry

    lax.fori_loop(0, n, rank_block, 0)

    def rows_of(sl):
        cell = (a_ref[0:1, sl] * 128 + b_ref[0:1, sl] + 1).astype(f32)
        return [p_ref[0:1, sl], p_ref[1:2, sl], cell]

    place_all(rows_of, HEAD, head_row, HEAD_ROWS, key_ref, rank_ref, count_ref[...], out_ref, acc_ref, left_ref, col_ref, hot_ref)

    side = around()
    height, width = v_ref.shape[1:]
    turned = [v_ref[c].T for c in range(2)]
    lane = lax.broadcasted_iota(i32, (1, width), 1)
    for dx in (-1, 0, 1):
        for dy in (-1, 0, 1):
            if dx == 0 and dy == 0:
                continue
            row = height - 1 if dx > 0 else 0
            col = width - 1 if dy > 0 else 0
            inside, who = side(dx, dy)
            base = who * HEAD_ROWS + HALO

            @pl.when(inside)
            def _():
                for c in range(2):
                    if dx:
                        line = v_ref[c, row:row + 1, :]
                        if dy:
                            one = jnp.sum(jnp.where(lane == col, line, 0.0), axis=1, keepdims=True)
                            line = jnp.broadcast_to(one, (1, width))
                        out_ref[pl.ds(base + c, 1), :] = line
                    else:
                        for h in range(2):
                            out_ref[pl.ds(base + 2 * c + h, 1), :] = turned[c][col:col + 1, h * 128:(h + 1) * 128]


def body_kernel(p_ref, key_ref, rank_ref, count_ref, out_ref, acc_ref, left_ref, col_ref, hot_ref):
    out_ref[...] = jnp.zeros(out_ref.shape, f32)

    def rows_of(sl):
        return [p_ref[k:k + 1, sl] for k in range(2, 8)]

    place_all(rows_of, BODY, body_row, BODY_ROWS, key_ref, rank_ref, count_ref[...], out_ref, acc_ref, left_ref, col_ref, hot_ref)


def quad(t):
    return 0.5 * t * (t - 1.0), 1.0 - t * t, 0.5 * t * (t + 1.0)


def pick_of(hits, values, zero):
    out = zero
    for h, v in reversed(list(zip(hits, values))):
        out = jnp.where(h, v, out)
    return out


def interp_kernel(r_ref, v_ref, out_ref, cell_ref, f_ref):
    S = 8
    side = around()

    def from_side(dx, dy, k):
        inside, who = side(dx, dy)
        row = r_ref[pl.ds(who * HEAD_ROWS + HALO + k, 1), :]
        return jnp.where(inside, row, 0.0)

    for c in range(2):
        hi, lo = split(v_ref[c].T)
        f_ref[c * 128:(c + 1) * 128, :] = hi
        f_ref[256 + c * 128:256 + (c + 1) * 128, :] = lo
    z4 = jnp.zeros((4, 128), f32)
    flat = jnp.concatenate([from_side(dx, 0, c) for c in range(2) for dx in (-1, 1)] + [z4], 0)
    west = jnp.concatenate([from_side(dx, -1, c) for c in range(2) for dx in (-1, 1)] + [z4], 0)
    east = jnp.concatenate([from_side(dx, 1, c) for c in range(2) for dx in (-1, 1)] + [z4], 0)
    tall = jnp.concatenate([from_side(0, dy, 2 * c + h) for h in range(2) for c in range(2) for dy in (-1, 1)], 0)
    sub = lax.broadcasted_iota(i32, (8, 128), 0)
    even = (sub & 1) == 0
    upper = sub < 4
    own = [(sub >> 1) == c for c in range(2)]
    own2 = [((sub >> 1) & 1) == c for c in range(2)]
    sub_f = sub.astype(f32)
    row_b = iota((16, 128), 0, bf16)
    zb = jnp.zeros((16, 128), bf16)
    z8 = jnp.zeros((8, 128), f32)

    def step(i, carry):
        groups = []
        for h in range(2):
            f, g, cell = [r_ref[pl.ds(i * (S * HEAD_ROWS) + head_row(k, h), S, stride=HEAD_ROWS), :] for k in range(3)]
            ci = cell.astype(i32) - 1
            cell_ref[pl.ds(i * (2 * S) + h, S, stride=2), :] = ci
            live = ci >= 0
            a = jnp.where(live, ci >> 7, 0)
            b = ci & 127
            half = jnp.where(live, 0.5, 0.0)
            wa = [half * w for w in quad(f)]
            wb = list(quad(g))
            hi = [w.astype(bf16).astype(f32) for w in wa]
            lo = [w - v for w, v in zip(wa, hi)]
            el, er = jnp.where(b == 0, wb[0], 0.0), jnp.where(b == 127, wb[2], 0.0)
            wb[0], wb[2] = wb[0] - el, wb[2] - er
            et, eb = jnp.where(a == 0, wa[0], 0.0), jnp.where(a == 255, wa[2], 0.0)
            at_a = [a - 1 + k for k in range(3)]
            w_half = [[jnp.where((t >> 7) == k, w, 0.0) for k in range(2)] for t, w in zip(at_a, wa)]
            groups.append(dict(
                w=hi + lo + [((a - 1) & 31).astype(f32), ((a - 1) >> 5).astype(f32)],
                wb=wb, start=((b - 1) & 7).astype(f32), q=((b - 1) >> 3) & 15, e=[el, er, et, eb],
                ia=[t & 127 for t in at_a], ib=[(b - 1 + k) & 127 for k in range(3)], w_half=w_half))

        def wide(x, j):
            return jnp.broadcast_to(x[j:j + 1], (8, 128))

        for u in range(S):
            spread = []
            for h in range(2):
                G = groups[h]
                packed = []
                for x in G["w"]:
                    y = wide(x, u)
                    packed.append(jnp.concatenate([y, y], 0).astype(bf16))
                his, los, start, q = packed[:3], packed[3:6], packed[6], packed[7]
                d = row_b - start
                near = [d == jnp.asarray(k, bf16) for k in range(3)]
                far = [d == jnp.asarray(k - 16, bf16) for k in range(3)]
                over = [d == jnp.asarray(k - 32, bf16) for k in (1, 2)]
                pieces = []
                for w in (his, los):
                    pieces.append((pick_of(near, w, zb), pick_of(far, w, zb), pick_of(over, w[1:], zb)))
                hit = q == jnp.asarray(-1, bf16)
                cols = [[], []]
                for j in range(8):
                    prev = hit
                    hit = q == jnp.asarray(j, bf16)
                    for k in range(2):
                        p0, p1, p2 = pieces[k]
                        cols[k].append(jnp.where(hit, p0, jnp.where(prev, p2, zb)))
                        cols[k].append(jnp.where(hit, p1, zb))
                spread.append([jnp.concatenate(c, 0) for c in cols])
            whi, wlo = [jnp.concatenate([spread[0][k], spread[1][k]], 1) for k in range(2)]
            two = nn(f_ref[...], whi)
            R = two[:256] + two[256:] + nn(f_ref[:256, :], wlo)
            for h in range(2):
                G = groups[h]
                V = R[:, 128 * h:128 * h + 128]
                d = sub_f - wide(G["start"], u)
                wb = [wide(w, u) for w in G["wb"]]
                c0 = pick_of([d == float(k) for k in range(3)], wb, z8)
                c1 = pick_of([d == float(k - 8) for k in (1, 2)], wb[1:], z8)
                q = wide(G["q"], u)
                bits = [(q & (1 << k)) != 0 for k in range(4)]

                def mux(v, b0, b1):
                    return jnp.where(b1, jnp.where(b0, v[3], v[2]), jnp.where(b0, v[1], v[0]))

                el, er, et, eb = [wide(e, u) for e in G["e"]]
                ga = [jnp.take_along_axis(tall, wide(t, u), axis=1) for t in G["ia"]]
                gb = [jnp.take_along_axis(flat, wide(t, u), axis=1) for t in G["ib"]]
                wh = [jnp.where(upper, wide(w[0], u), wide(w[1], u)) for w in G["w_half"]]
                beside = (wh[0] * ga[0] + wh[1] * ga[1] + wh[2] * ga[2]) * jnp.where(even, el, er)
                along = (wb[0] * gb[0] + wb[1] * gb[1] + wb[2] * gb[2] + el * west + er * east) * jnp.where(even, et, eb)
                for c in range(2):
                    r = [V[c * 128 + 8 * j:c * 128 + 8 * j + 8] for j in range(16)]
                    e = [mux([r[4 * m + t] for m in range(4)], bits[2], bits[3]) for t in range(4)]
                    e.append(mux([r[(4 * m + 4) % 16] for m in range(4)], bits[2], bits[3]))
                    first = mux(e[:4], bits[0], bits[1])
                    second = mux(e[1:], bits[0], bits[1])
                    total = first * c0 + second * c1 + jnp.where(own2[c], beside, 0.0) + jnp.where(own[c], along, 0.0)
                    row = PAD + 2 * (2 * u + h) + c
                    out_ref[pl.ds(i * (4 * S) + row, 1), :] = jnp.sum(total, axis=0, keepdims=True)
        return carry

    lax.fori_loop(0, OWNERS // S, step, 0)


def merge_kernel(d_ref, r1_ref, r2_ref, out_ref):
    S = out_ref.shape[1] // 256
    s0 = pl.program_id(0) * S
    sub = lax.broadcasted_iota(i32, (8, 128), 0)
    top, mid = sub < 2, sub < 4
    lead = pltpu.roll(r2_ref[0:8, :], 2, 0)
    for s in range(S):
        for h in range(2):
            src = s0 + s
            w = r1_ref[pl.ds(src * HEAD_ROWS + 2 * h, 8), :]
            at = src * BODY_ROWS + BODY * h - 2
            if s == 0 and h == 0:
                u = jnp.where(s0 == 0, lead, r2_ref[pl.ds(jnp.maximum(at, 0), 8), :])
            else:
                u = r2_ref[pl.ds(at, 8), :]
            d = d_ref[pl.ds(PAD + 2 * (2 * src + h) - 2, 8), :]
            out_ref[:, s * 256 + h * 128:s * 256 + h * 128 + 128] = jnp.where(top, w, jnp.where(mid, u + d, u))


def shape(*dims, dt=f32):
    return jax.ShapeDtypeStruct(dims, dt)


def scratch(width):
    return [pltpu.VMEM((64 * width, 256), f32), pltpu.VMEM((128 * width, PB), bf16), pltpu.VMEM((256, PB), bf16), pltpu.VMEM((128, 128), f32)]


def head(particles, key, a, b, velocity):
    n = particles.shape[1]
    return pl.pallas_call(
        head_kernel,
        out_shape=(shape(OWNERS * HEAD_ROWS, 128), shape(1, n), shape(128, 128)),
        in_specs=[VMEM] * 5,
        out_specs=(VMEM,) * 3,
        scratch_shapes=scratch(HEAD) + [pltpu.VMEM((128, 256), bf16), pltpu.VMEM((RB, 128), bf16)],
        name="head",
    )(particles, key, a, b, velocity)


def body(particles, key, rank, count):
    return pl.pallas_call(
        body_kernel,
        out_shape=shape(OWNERS * BODY_ROWS, 128),
        in_specs=[VMEM] * 4,
        out_specs=VMEM,
        scratch_shapes=scratch(BODY),
        name="body",
    )(particles, key, rank, count)


def interp(arrived, velocity):
    return pl.pallas_call(
        interp_kernel,
        out_shape=(shape(PAD + 4 * OWNERS + 8, 128), shape(2 * OWNERS, 128, dt=i32)),
        in_specs=[VMEM] * 2,
        out_specs=(VMEM,) * 2,
        scratch_shapes=[pltpu.VMEM((512, 256), bf16)],
        name="interp",
    )(arrived, velocity)


def merge(moved, head_arrived, body_arrived):
    n = OWNERS * 256
    g = 8
    return pl.pallas_call(
        merge_kernel,
        out_shape=shape(8, n),
        grid=(g,),
        in_specs=[VMEM] * 3,
        out_specs=pl.BlockSpec((8, n // g), lambda i: (0, i)),
        name="merge",
    )(moved, head_arrived, body_arrived)


def exchange(buckets, rows):
    out = lax.all_to_all(buckets.reshape(OWNERS, rows, 1, 128), ALL, 0, 0, tiled=True)
    return out.reshape(OWNERS * rows, 128)


def shards(particles, dest_key, cell_a, cell_b, velocity):
    key, a, b = [v.reshape(1, -1) for v in (dest_key, cell_a, cell_b)]
    first, rank, count = head(particles, key, a, b, velocity)
    arrived = exchange(first, HEAD_ROWS)
    rest = exchange(body(particles, key, rank, count), BODY_ROWS)
    moved, cell = interp(arrived, velocity)
    return merge(moved, arrived, rest), cell.reshape(-1)


def solution(mesh):
    split_mesh = Mesh(mesh.devices.reshape(mesh.shape["gx"], 4, 4, mesh.shape["gz"]), ALL)
    in_specs = (P(None, ALL), P(ALL), P(ALL), P(ALL), P(None, "gx", WIDE))
    out_specs = (P(None, ALL), P(ALL))
    return jax.shard_map(shards, mesh=split_mesh, in_specs=in_specs, out_specs=out_specs, check_vma=False)
```

```python
import jax
import jax.numpy as jnp
from jax import lax
from jax.experimental import pallas as pl
from jax.experimental.pallas import tpu as pltpu
from jax.sharding import Mesh
from jax.sharding import PartitionSpec as P

f32, bf16, i32 = jnp.float32, jnp.bfloat16, jnp.int32
ALL = ("gx", "gy_0", "gy_1", "gz")
WIDE = ("gy_0", "gy_1", "gz")
OWNERS = 128
HEAD = 3
BODY = 6
HEAD_ROWS = 10
BODY_ROWS = 12
HALO = 6
PAD = 8
PB = 4096
RB = 4096
VMEM = pl.BlockSpec(memory_space=pltpu.VMEM)


def iota(shape, dim, dt):
    return lax.broadcasted_iota(i32, shape, dim).astype(f32).astype(dt)


def nt(a, b):
    return lax.dot_general(a, b, (((1,), (1,)), ((), ())), preferred_element_type=f32)


def nn(a, b):
    return jnp.dot(a, b, preferred_element_type=f32)


def split(v):
    hi = v.astype(bf16)
    return hi, (v - hi.astype(f32)).astype(bf16)


def one_hot(size, t):
    hit = iota((size, t.shape[1]), 0, bf16) == t.astype(bf16)
    return jnp.where(hit, jnp.ones((), bf16), jnp.zeros((), bf16))


def block(i, size):
    if isinstance(i, int):
        return slice(i * size, (i + 1) * size)
    return pl.ds(pl.multiple_of(i * size, size), size)


def column_of(key, rank, first):
    off = rank - first
    fits = (off >= 0.0) & (off < 128.0)
    return jnp.where(fits, off + jnp.where(key >= 64, 128.0, 0.0), -1.0)


def head_row(k, half):
    return 2 * half + k if k < 2 else 4 + half


def body_row(k, half):
    return BODY * half + k


def place_all(rows_of, width, row_at, stride, key_ref, rank_ref, counts, out_ref, acc_ref, left_ref, col_ref, hot_ref):
    n = key_ref.shape[1] // PB
    m = 64 * width
    ids = lax.broadcasted_iota(i32, (128, 128), 0).astype(f32)
    n_full = jnp.max(jnp.sum(jnp.where(counts > 128.0, 1.0, 0.0), axis=0, keepdims=True))
    hot = jnp.max(jnp.where(counts > 128.0, ids, -1.0)).astype(i32)
    few = n_full <= 1.0
    hot_key = jnp.where(few, hot, -1)

    def add_placed(rows, key, t):
        pick = one_hot(64, jnp.where(key >= 64, key - 64, key).astype(f32))
        for k, r in enumerate(rows):
            hi, lo = split(r)
            left_ref[k * 64:(k + 1) * 64, :] = pick * hi
            left_ref[m + k * 64:m + (k + 1) * 64, :] = pick * lo
        col_ref[...] = one_hot(256, t)
        both = nt(left_ref[...], col_ref[...])
        acc_ref[...] += both[:m] + both[m:]

    def flush(half):
        for k in range(width):
            for o in range(2):
                at = pl.ds(o * 64 * stride + row_at(k, half), 64, stride=stride)
                out_ref[at, :] = acc_ref[k * 64:(k + 1) * 64, o * 128:(o + 1) * 128]

    acc_ref[...] = jnp.zeros(acc_ref.shape, f32)
    hot_ref[...] = jnp.zeros(hot_ref.shape, f32)

    def step(i, carry):
        sl = block(i, PB)
        key, rank = key_ref[0:1, sl], rank_ref[0:1, sl]
        rows = rows_of(sl)
        add_placed(rows, key, column_of(key, rank, 0.0))
        over = jnp.where(key == hot_key, rank - 128.0, -1.0)
        hi, lo = split(jnp.concatenate(rows + [jnp.zeros((8 - width, PB), f32)], 0))
        hot_ref[:, :16] += nt(one_hot(128, over), jnp.concatenate([hi, lo], 0))
        return carry

    for i in range(n):
        step(i, 0)
    flush(0)
    turned = hot_ref[...].T
    spill = turned[:8] + turned[8:16]
    base = jnp.maximum(hot, 0) * stride
    for k in range(width):
        out_ref[pl.ds(base + row_at(k, 1), 1), :] = spill[k:k + 1]

    @pl.when(jnp.logical_not(few))
    def _():
        acc_ref[...] = jnp.zeros(acc_ref.shape, f32)

        def again(i, carry):
            sl = block(i, PB)
            key = key_ref[0:1, sl]
            add_placed(rows_of(sl), key, column_of(key, rank_ref[0:1, sl], 128.0))
            return carry

        lax.fori_loop(0, n, again, 0)
        flush(1)


def around():
    x, y = lax.axis_index("gx"), lax.axis_index(WIDE)
    nx, ny = lax.axis_size("gx"), lax.axis_size(WIDE)

    def side(dx, dy):
        inside = (x + dx >= 0) & (x + dx < nx) & (y + dy >= 0) & (y + dy < ny)
        return inside, jnp.where(inside, (x + dx) * ny + y + dy, 0)

    return side


def head_kernel(p_ref, key_ref, a_ref, b_ref, v_ref, out_ref, rank_ref, count_ref, acc_ref, left_ref, col_ref, hot_ref, ut_ref, oh_ref):
    n = p_ref.shape[1] // RB
    out_ref[...] = jnp.zeros(out_ref.shape, f32)
    count_ref[...] = jnp.zeros(count_ref.shape, f32)
    before = lax.broadcasted_iota(i32, (128, 128), 0) < lax.broadcasted_iota(i32, (128, 128), 1)
    ut_ref[:, :128] = jnp.where(before, 1.0, 0.0).astype(bf16)
    ut_ref[:, 128:] = jnp.ones((128, 128), bf16)

    def rank_block(i, carry):
        sl = block(i, RB)
        key = key_ref[0:1, sl].astype(f32)
        for k in range(RB // 128):
            oh_ref[k * 128:(k + 1) * 128, :] = one_hot(128, key[:, k * 128:(k + 1) * 128])
        res = nn(oh_ref[...], ut_ref[...])
        base = count_ref[...]
        ranks = []
        for k in range(RB // 128):
            r = res[k * 128:(k + 1) * 128]
            hot = oh_ref[k * 128:(k + 1) * 128, :].astype(f32)
            ranks.append(jnp.sum(hot * (r[:, :128] + base), axis=0, keepdims=True))
            base = base + r[:, 128:]
        count_ref[...] = base
        rank_ref[0:1, sl] = jnp.concatenate(ranks, 1)
        return carry

    for i in range(n):
        rank_block(i, 0)

    def rows_of(sl):
        cell = (a_ref[0:1, sl] * 128 + b_ref[0:1, sl] + 1).astype(f32)
        return [p_ref[0:1, sl], p_ref[1:2, sl], cell]

    place_all(rows_of, HEAD, head_row, HEAD_ROWS, key_ref, rank_ref, count_ref[...], out_ref, acc_ref, left_ref, col_ref, hot_ref)

    side = around()
    height, width = v_ref.shape[1:]
    turned = [v_ref[c].T for c in range(2)]
    for dx in (-1, 0, 1):
        for dy in (-1, 0, 1):
            if dx == 0 and dy == 0:
                continue
            row = height - 1 if dx > 0 else 0
            col = width - 1 if dy > 0 else 0
            inside, who = side(dx, dy)
            base = who * HEAD_ROWS + HALO

            @pl.when(inside)
            def _():
                for c in range(2):
                    if dx:
                        out_ref[pl.ds(base + c, 1), :] = v_ref[c, row:row + 1, :]
                    else:
                        for h in range(2):
                            out_ref[pl.ds(base + 2 * c + h, 1), :] = turned[c][col:col + 1, h * 128:(h + 1) * 128]


def body_kernel(p_ref, key_ref, rank_ref, count_ref, out_ref, acc_ref, left_ref, col_ref, hot_ref):
    out_ref[...] = jnp.zeros(out_ref.shape, f32)

    def rows_of(sl):
        return [p_ref[k:k + 1, sl] for k in range(2, 8)]

    place_all(rows_of, BODY, body_row, BODY_ROWS, key_ref, rank_ref, count_ref[...], out_ref, acc_ref, left_ref, col_ref, hot_ref)


def quad(t):
    return 0.5 * t * (t - 1.0), 1.0 - t * t, 0.5 * t * (t + 1.0)


def pick_of(hits, values, zero):
    out = zero
    for h, v in reversed(list(zip(hits, values))):
        out = jnp.where(h, v, out)
    return out


def interp_kernel(r_ref, v_ref, out_ref, cell_ref, f_ref):
    S = 8
    side = around()

    def from_side(dx, dy, k):
        inside, who = side(dx, dy)
        row = r_ref[pl.ds(who * HEAD_ROWS + HALO + k, 1), :]
        return jnp.where(inside, row, 0.0)

    for c in range(2):
        hi, lo = split(v_ref[c].T)
        f_ref[c * 128:(c + 1) * 128, :] = hi
        f_ref[256 + c * 128:256 + (c + 1) * 128, :] = lo
    z4 = jnp.zeros((4, 128), f32)
    flat = jnp.concatenate([from_side(dx, 0, c) for c in range(2) for dx in (-1, 1)] + [z4], 0)
    west = jnp.concatenate([from_side(dx, -1, c) for c in range(2) for dx in (-1, 1)] + [z4], 0)
    east = jnp.concatenate([from_side(dx, 1, c) for c in range(2) for dx in (-1, 1)] + [z4], 0)
    west = jnp.broadcast_to(west[:, 127:128], (8, 128))
    east = jnp.broadcast_to(east[:, 0:1], (8, 128))
    tall = jnp.concatenate([from_side(0, dy, 2 * c + h) for h in range(2) for c in range(2) for dy in (-1, 1)], 0)
    sub = lax.broadcasted_iota(i32, (8, 128), 0)
    even = (sub & 1) == 0
    upper = sub < 4
    own = [(sub >> 1) == c for c in range(2)]
    own2 = [((sub >> 1) & 1) == c for c in range(2)]
    sub_f = sub.astype(f32)
    row_b = iota((16, 128), 0, bf16)
    zb = jnp.zeros((16, 128), bf16)
    z8 = jnp.zeros((8, 128), f32)

    def step(i, carry):
        groups = []
        for h in range(2):
            f, g, cell = [r_ref[pl.ds(i * (S * HEAD_ROWS) + head_row(k, h), S, stride=HEAD_ROWS), :] for k in range(3)]
            ci = cell.astype(i32) - 1
            cell_ref[pl.ds(i * (2 * S) + h, S, stride=2), :] = ci
            live = ci >= 0
            a = jnp.where(live, ci >> 7, 0)
            b = ci & 127
            half = jnp.where(live, 0.5, 0.0)
            wa = [half * w for w in quad(f)]
            wb = list(quad(g))
            hi = [w.astype(bf16).astype(f32) for w in wa]
            lo = [w - v for w, v in zip(wa, hi)]
            el, er = jnp.where(b == 0, wb[0], 0.0), jnp.where(b == 127, wb[2], 0.0)
            wb[0], wb[2] = wb[0] - el, wb[2] - er
            et, eb = jnp.where(a == 0, wa[0], 0.0), jnp.where(a == 255, wa[2], 0.0)
            at_a = [a - 1 + k for k in range(3)]
            w_half = [[jnp.where((t >> 7) == k, w, 0.0) for k in range(2)] for t, w in zip(at_a, wa)]
            groups.append(dict(
                w=hi + lo + [((a - 1) & 31).astype(f32), ((a - 1) >> 5).astype(f32)],
                wb=wb, start=((b - 1) & 7).astype(f32), q=((b - 1) >> 3) & 15, e=[el, er, et, eb],
                ia=[t & 127 for t in at_a], ib=[(b - 1 + k) & 127 for k in range(3)], w_half=w_half))

        def wide(x, j):
            return jnp.broadcast_to(x[j:j + 1], (8, 128))

        for u in range(S):
            spread = []
            for h in range(2):
                G = groups[h]
                packed = []
                for x in G["w"]:
                    y = wide(x, u)
                    packed.append(jnp.concatenate([y, y], 0).astype(bf16))
                his, los, start, q = packed[:3], packed[3:6], packed[6], packed[7]
                d = row_b - start
                near = [d == jnp.asarray(k, bf16) for k in range(3)]
                far = [d == jnp.asarray(k - 16, bf16) for k in range(3)]
                over = [d == jnp.asarray(k - 32, bf16) for k in (1, 2)]
                pieces = []
                for w in (his, los):
                    pieces.append((pick_of(near, w, zb), pick_of(far, w, zb), pick_of(over, w[1:], zb)))
                hit = q == jnp.asarray(-1, bf16)
                cols = [[], []]
                for j in range(8):
                    prev = hit
                    hit = q == jnp.asarray(j, bf16)
                    for k in range(2):
                        p0, p1, p2 = pieces[k]
                        cols[k].append(jnp.where(hit, p0, jnp.where(prev, p2, zb)))
                        cols[k].append(jnp.where(hit, p1, zb))
                spread.append([jnp.concatenate(c, 0) for c in cols])
            whi, wlo = [jnp.concatenate([spread[0][k], spread[1][k]], 1) for k in range(2)]
            two = nn(f_ref[...], whi)
            R = two[:256] + two[256:] + nn(f_ref[:256, :], wlo)
            for h in range(2):
                G = groups[h]
                V = R[:, 128 * h:128 * h + 128]
                d = sub_f - wide(G["start"], u)
                wb = [wide(w, u) for w in G["wb"]]
                c0 = pick_of([d == float(k) for k in range(3)], wb, z8)
                c1 = pick_of([d == float(k - 8) for k in (1, 2)], wb[1:], z8)
                q = wide(G["q"], u)
                bits = [(q & (1 << k)) != 0 for k in range(4)]

                def mux(v, b0, b1):
                    return jnp.where(b1, jnp.where(b0, v[3], v[2]), jnp.where(b0, v[1], v[0]))

                el, er, et, eb = [wide(e, u) for e in G["e"]]
                ga = [jnp.take_along_axis(tall, wide(t, u), axis=1) for t in G["ia"]]
                gb = [jnp.take_along_axis(flat, wide(t, u), axis=1) for t in G["ib"]]
                wh = [jnp.where(upper, wide(w[0], u), wide(w[1], u)) for w in G["w_half"]]
                beside = (wh[0] * ga[0] + wh[1] * ga[1] + wh[2] * ga[2]) * jnp.where(even, el, er)
                along = (wb[0] * gb[0] + wb[1] * gb[1] + wb[2] * gb[2] + el * west + er * east) * jnp.where(even, et, eb)
                for c in range(2):
                    r = [V[c * 128 + 8 * j:c * 128 + 8 * j + 8] for j in range(16)]
                    e = [mux([r[4 * m + t] for m in range(4)], bits[2], bits[3]) for t in range(4)]
                    e.append(mux([r[(4 * m + 4) % 16] for m in range(4)], bits[2], bits[3]))
                    first = mux(e[:4], bits[0], bits[1])
                    second = mux(e[1:], bits[0], bits[1])
                    total = first * c0 + second * c1 + jnp.where(own2[c], beside, 0.0) + jnp.where(own[c], along, 0.0)
                    row = PAD + 2 * (2 * u + h) + c
                    out_ref[pl.ds(i * (4 * S) + row, 1), :] = jnp.sum(total, axis=0, keepdims=True)
        return carry

    lax.fori_loop(0, OWNERS // S, step, 0)


def merge_kernel(d_ref, r1_ref, r2_ref, out_ref):
    S = out_ref.shape[1] // 256
    s0 = pl.program_id(0) * S
    sub = lax.broadcasted_iota(i32, (8, 128), 0)
    top, mid = sub < 2, sub < 4
    lead = pltpu.roll(r2_ref[0:8, :], 2, 0)
    for s in range(S):
        for h in range(2):
            src = s0 + s
            w = r1_ref[pl.ds(src * HEAD_ROWS + 2 * h, 8), :]
            at = src * BODY_ROWS + BODY * h - 2
            if s == 0 and h == 0:
                u = jnp.where(s0 == 0, lead, r2_ref[pl.ds(jnp.maximum(at, 0), 8), :])
            else:
                u = r2_ref[pl.ds(at, 8), :]
            d = d_ref[pl.ds(PAD + 2 * (2 * src + h) - 2, 8), :]
            out_ref[:, s * 256 + h * 128:s * 256 + h * 128 + 128] = jnp.where(top, w, jnp.where(mid, u + d, u))


def shape(*dims, dt=f32):
    return jax.ShapeDtypeStruct(dims, dt)


def held(*dims, dt=f32):
    return pltpu.VMEM(dims, dt)


def near_memory(x):
    return pltpu.with_memory_space_constraint(x, pltpu.VMEM)


def scratch(width):
    return [pltpu.VMEM((64 * width, 256), f32), pltpu.VMEM((128 * width, PB), bf16), pltpu.VMEM((256, PB), bf16), pltpu.VMEM((128, 128), f32)]


def head(particles, key, a, b, velocity):
    n = particles.shape[1]
    return pl.pallas_call(
        head_kernel,
        out_shape=(held(OWNERS * HEAD_ROWS, 128), held(1, n), held(128, 128)),
        in_specs=[VMEM] * 5,
        out_specs=(VMEM,) * 3,
        scratch_shapes=scratch(HEAD) + [pltpu.VMEM((128, 256), bf16), pltpu.VMEM((RB, 128), bf16)],
        name="head",
    )(particles, key, a, b, velocity)


def body(particles, key, rank, count):
    return pl.pallas_call(
        body_kernel,
        out_shape=held(OWNERS * BODY_ROWS, 128),
        in_specs=[VMEM] * 4,
        out_specs=VMEM,
        scratch_shapes=scratch(BODY),
        name="body",
    )(particles, key, near_memory(rank), near_memory(count))


def interp(arrived, velocity):
    return pl.pallas_call(
        interp_kernel,
        out_shape=(held(PAD + 4 * OWNERS + 8, 128), shape(2 * OWNERS, 128, dt=i32)),
        in_specs=[VMEM] * 2,
        out_specs=(VMEM,) * 2,
        scratch_shapes=[pltpu.VMEM((512, 256), bf16)],
        name="interp",
    )(arrived, velocity)


def merge(moved, head_arrived, body_arrived):
    n = OWNERS * 256
    g = 8
    return pl.pallas_call(
        merge_kernel,
        out_shape=shape(8, n),
        grid=(g,),
        in_specs=[VMEM] * 3,
        out_specs=pl.BlockSpec((8, n // g), lambda i: (0, i)),
        name="merge",
    )(near_memory(moved), head_arrived, body_arrived)


def exchange(buckets, rows):
    out = lax.all_to_all(buckets.reshape(OWNERS, rows, 1, 128), ALL, 0, 0, tiled=True)
    return near_memory(out.reshape(OWNERS * rows, 128))


def shards(particles, dest_key, cell_a, cell_b, velocity):
    key, a, b = [v.reshape(1, -1) for v in (dest_key, cell_a, cell_b)]
    first, rank, count = head(particles, key, a, b, velocity)
    arrived = exchange(first, HEAD_ROWS)
    rest = exchange(body(particles, key, rank, count), BODY_ROWS)
    moved, cell = interp(arrived, velocity)
    return merge(moved, arrived, rest), cell.reshape(-1)


def solution(mesh):
    split_mesh = Mesh(mesh.devices.reshape(mesh.shape["gx"], 4, 4, mesh.shape["gz"]), ALL)
    in_specs = (P(None, ALL), P(ALL), P(ALL), P(ALL), P(None, "gx", WIDE))
    out_specs = (P(None, ALL), P(ALL))
    return jax.shard_map(shards, mesh=split_mesh, in_specs=in_specs, out_specs=out_specs, check_vma=False)
```

```python
import jax
import jax.numpy as jnp
from jax import lax
from jax.experimental import pallas as pl
from jax.experimental.pallas import tpu as pltpu
from jax.sharding import Mesh
from jax.sharding import PartitionSpec as P

f32, bf16, i32 = jnp.float32, jnp.bfloat16, jnp.int32
ALL = ("gx", "gy_0", "gy_1", "gz")
WIDE = ("gy_0", "gy_1", "gz")
OWNERS = 128
HEAD = 3
BODY = 6
HEAD_ROWS = 10
BODY_ROWS = 12
HALO = 6
PAD = 8
PB = 4096
RB = 4096
VMEM = pl.BlockSpec(memory_space=pltpu.VMEM)


def iota(shape, dim, dt):
    return lax.broadcasted_iota(i32, shape, dim).astype(f32).astype(dt)


def nt(a, b):
    return lax.dot_general(a, b, (((1,), (1,)), ((), ())), preferred_element_type=f32)


def nn(a, b):
    return jnp.dot(a, b, preferred_element_type=f32)


def split(v):
    hi = v.astype(bf16)
    return hi, (v - hi.astype(f32)).astype(bf16)


def one_hot(size, t):
    hit = iota((size, t.shape[1]), 0, bf16) == t.astype(bf16)
    return jnp.where(hit, jnp.ones((), bf16), jnp.zeros((), bf16))


def block(i, size):
    if isinstance(i, int):
        return slice(i * size, (i + 1) * size)
    return pl.ds(pl.multiple_of(i * size, size), size)


def column_of(key, rank, first):
    off = rank - first
    fits = (off >= 0.0) & (off < 128.0)
    return jnp.where(fits, off + jnp.where(key >= 64, 128.0, 0.0), -1.0)


def head_row(k, half):
    return 2 * half + k if k < 2 else 4 + half


def body_row(k, half):
    return BODY * half + k


def place_all(rows_of, width, row_at, stride, key_ref, rank_ref, counts, out_ref, acc_ref, left_ref, col_ref, hot_ref):
    n = key_ref.shape[1] // PB
    m = 64 * width
    ids = lax.broadcasted_iota(i32, (128, 128), 0).astype(f32)
    n_full = jnp.sum(jnp.where(counts > 128.0, 1.0, 0.0), axis=0, keepdims=True)
    hot = jnp.max(jnp.where(counts > 128.0, ids, -1.0), axis=0, keepdims=True)
    lone = jnp.concatenate([jnp.where(n_full <= 1.0, hot, -1.0)] * (PB // 128), 1)

    def fill(rows, low, t):
        pick = one_hot(64, low)
        for k, r in enumerate(rows):
            hi, lo = split(r)
            left_ref[k * 64:(k + 1) * 64, :] = pick * hi
            left_ref[m + k * 64:m + (k + 1) * 64, :] = pick * lo
        col_ref[...] = one_hot(256, t)

    def flush(half):
        for k in range(width):
            for o in range(2):
                at = pl.ds(o * 64 * stride + row_at(k, half), 64, stride=stride)
                out_ref[at, :] = acc_ref[k * 64:(k + 1) * 64, o * 128:(o + 1) * 128]

    acc_ref[...] = jnp.zeros(acc_ref.shape, f32)
    hot_ref[...] = jnp.zeros(hot_ref.shape, f32)
    for i in range(n):
        sl = block(i, PB)
        key, rank = key_ref[0:1, sl], rank_ref[0:1, sl]
        rows = rows_of(sl)
        over = (key.astype(f32) == lone) & (rank >= 128.0)
        low = jnp.where(over, -1.0, (key & 63).astype(f32))
        fill(rows, low, jnp.where(over, rank - 128.0, column_of(key, rank, 0.0)))
        tail = jnp.concatenate([jnp.where(over, r, 0.0) for r in rows] + [jnp.zeros((8 - width, PB), f32)], 0)
        hi = tail.astype(bf16).astype(f32)
        left_ref[2 * m:, :] = jnp.concatenate([hi, tail - hi], 0).astype(bf16)
        both = nt(left_ref[...], col_ref[...])
        acc_ref[...] += both[:m] + both[m:2 * m]
        hot_ref[...] += (both[2 * m:2 * m + 8] + both[2 * m + 8:])[:, :128]
    flush(0)
    base = jnp.max(jnp.maximum(hot, 0.0)).astype(i32) * stride
    for k in range(width):
        out_ref[pl.ds(base + row_at(k, 1), 1), :] = hot_ref[k:k + 1, :]

    @pl.when(jnp.max(n_full) > 1.0)
    def _():
        acc_ref[...] = jnp.zeros(acc_ref.shape, f32)

        def again(i, carry):
            sl = block(i, PB)
            key = key_ref[0:1, sl]
            fill(rows_of(sl), (key & 63).astype(f32), column_of(key, rank_ref[0:1, sl], 128.0))
            both = nt(left_ref[:2 * m, :], col_ref[...])
            acc_ref[...] += both[:m] + both[m:]
            return carry

        lax.fori_loop(0, n, again, 0)
        flush(1)


def around():
    x, y = lax.axis_index("gx"), lax.axis_index(WIDE)
    nx, ny = lax.axis_size("gx"), lax.axis_size(WIDE)

    def side(dx, dy):
        inside = (x + dx >= 0) & (x + dx < nx) & (y + dy >= 0) & (y + dy < ny)
        return inside, jnp.where(inside, (x + dx) * ny + y + dy, 0)

    return side


def head_kernel(p_ref, key_ref, a_ref, b_ref, v_ref, out_ref, rank_ref, count_ref, acc_ref, left_ref, col_ref, hot_ref, ut_ref, oh_ref):
    n = p_ref.shape[1] // RB
    out_ref[...] = jnp.zeros(out_ref.shape, f32)
    before = lax.broadcasted_iota(i32, (256, 256), 0) < lax.broadcasted_iota(i32, (256, 256), 1)
    ut_ref[...] = jnp.where(before, 1.0, 0.0).astype(bf16)
    base = jnp.zeros((128, 1), f32)
    for i in range(n):
        key = key_ref[0:1, block(i, RB)].astype(f32)
        for k in range(RB // 256):
            oh_ref[k * 128:(k + 1) * 128, :] = one_hot(128, key[:, k * 256:(k + 1) * 256])
        res = nn(oh_ref[...], ut_ref[...])
        ranks = []
        for k in range(RB // 256):
            hot = oh_ref[k * 128:(k + 1) * 128, :].astype(f32)
            ranks.append(jnp.sum(hot * (res[k * 128:(k + 1) * 128] + base), axis=0, keepdims=True))
            base = base + jnp.sum(hot, axis=1, keepdims=True)
        rank_ref[0:1, block(i, RB)] = jnp.concatenate(ranks, 1)
    count_ref[...] = jnp.broadcast_to(base, (128, 128))

    def rows_of(sl):
        cell = (a_ref[0:1, sl] * 128 + b_ref[0:1, sl] + 1).astype(f32)
        return [p_ref[0:1, sl], p_ref[1:2, sl], cell]

    place_all(rows_of, HEAD, head_row, HEAD_ROWS, key_ref, rank_ref, count_ref[...], out_ref, acc_ref, left_ref, col_ref, hot_ref)

    side = around()
    height, width = v_ref.shape[1:]
    turned = [v_ref[c].T for c in range(2)]
    for dx in (-1, 0, 1):
        for dy in (-1, 0, 1):
            if dx == 0 and dy == 0:
                continue
            row = height - 1 if dx > 0 else 0
            col = width - 1 if dy > 0 else 0
            inside, who = side(dx, dy)
            base = who * HEAD_ROWS + HALO

            @pl.when(inside)
            def _():
                for c in range(2):
                    if dx:
                        out_ref[pl.ds(base + c, 1), :] = v_ref[c, row:row + 1, :]
                    else:
                        for h in range(2):
                            out_ref[pl.ds(base + 2 * c + h, 1), :] = turned[c][col:col + 1, h * 128:(h + 1) * 128]


def body_kernel(p_ref, key_ref, rank_ref, count_ref, v_ref, out_ref, f_ref, acc_ref, left_ref, col_ref, hot_ref):
    out_ref[...] = jnp.zeros(out_ref.shape, f32)
    for c in range(2):
        hi, lo = split(v_ref[c].T)
        f_ref[c * 128:(c + 1) * 128, :] = hi
        f_ref[256 + c * 128:256 + (c + 1) * 128, :] = lo

    def rows_of(sl):
        return [p_ref[k:k + 1, sl] for k in range(2, 8)]

    place_all(rows_of, BODY, body_row, BODY_ROWS, key_ref, rank_ref, count_ref[...], out_ref, acc_ref, left_ref, col_ref, hot_ref)


def quad(t):
    return 0.5 * t * (t - 1.0), 1.0 - t * t, 0.5 * t * (t + 1.0)


def pick_of(hits, values, zero):
    out = zero
    for h, v in reversed(list(zip(hits, values))):
        out = jnp.where(h, v, out)
    return out


def interp_kernel(r_ref, f_ref, out_ref, cell_ref):
    S = 16
    side = around()

    def from_side(dx, dy, k):
        inside, who = side(dx, dy)
        row = r_ref[pl.ds(who * HEAD_ROWS + HALO + k, 1), :]
        return jnp.where(inside, row, 0.0)

    z4 = jnp.zeros((4, 128), f32)
    flat = jnp.concatenate([from_side(dx, 0, c) for c in range(2) for dx in (-1, 1)] + [z4], 0)
    west = jnp.concatenate([from_side(dx, -1, c) for c in range(2) for dx in (-1, 1)] + [z4], 0)
    east = jnp.concatenate([from_side(dx, 1, c) for c in range(2) for dx in (-1, 1)] + [z4], 0)
    west = jnp.broadcast_to(west[:, 127:128], (8, 128))
    east = jnp.broadcast_to(east[:, 0:1], (8, 128))
    tall = jnp.concatenate([from_side(0, dy, 2 * c + h) for h in range(2) for c in range(2) for dy in (-1, 1)], 0)
    sub = lax.broadcasted_iota(i32, (8, 128), 0)
    even = (sub & 1) == 0
    upper = sub < 4
    own = [(sub >> 1) == c for c in range(2)]
    own2 = [((sub >> 1) & 1) == c for c in range(2)]
    sub_f = sub.astype(f32)
    row_b = iota((16, 128), 0, bf16)
    zb = jnp.zeros((16, 128), bf16)
    z8 = jnp.zeros((8, 128), f32)

    def step(i, carry):
        groups = []
        for h in range(2):
            f, g, cell = [r_ref[pl.ds(i * (S * HEAD_ROWS) + head_row(k, h), S, stride=HEAD_ROWS), :] for k in range(3)]
            ci = cell.astype(i32) - 1
            cell_ref[pl.ds(i * (2 * S) + h, S, stride=2), :] = ci
            live = ci >= 0
            a = jnp.where(live, ci >> 7, 0)
            b = ci & 127
            half = jnp.where(live, 0.5, 0.0)
            wa = [half * w for w in quad(f)]
            wb = list(quad(g))
            hi = [w.astype(bf16).astype(f32) for w in wa]
            lo = [w - v for w, v in zip(wa, hi)]
            el, er = jnp.where(b == 0, wb[0], 0.0), jnp.where(b == 127, wb[2], 0.0)
            wb[0], wb[2] = wb[0] - el, wb[2] - er
            et, eb = jnp.where(a == 0, wa[0], 0.0), jnp.where(a == 255, wa[2], 0.0)
            at_a = [a - 1 + k for k in range(3)]
            w_half = [[jnp.where((t >> 7) == k, w, 0.0) for k in range(2)] for t, w in zip(at_a, wa)]
            groups.append(dict(
                w=hi + lo + [((a - 1) & 31).astype(f32), ((a - 1) >> 5).astype(f32)],
                wb=wb, start=((b - 1) & 7).astype(f32), q=((b - 1) >> 3) & 15, e=[el, er, et, eb],
                ia=[t & 127 for t in at_a], ib=[(b - 1 + k) & 127 for k in range(3)], w_half=w_half))

        def wide(x, j):
            return jnp.broadcast_to(x[j:j + 1], (8, 128))

        for u in range(S):
            spread = []
            for h in range(2):
                G = groups[h]
                packed = []
                for x in G["w"]:
                    y = wide(x, u)
                    packed.append(jnp.concatenate([y, y], 0).astype(bf16))
                his, los, start, q = packed[:3], packed[3:6], packed[6], packed[7]
                d = row_b - start
                near = [d == jnp.asarray(k, bf16) for k in range(3)]
                far = [d == jnp.asarray(k - 16, bf16) for k in range(3)]
                over = [d == jnp.asarray(k - 32, bf16) for k in (1, 2)]
                pieces = []
                for w in (his, los):
                    pieces.append((pick_of(near, w, zb), pick_of(far, w, zb), pick_of(over, w[1:], zb)))
                hit = q == jnp.asarray(-1, bf16)
                cols = [[], []]
                for j in range(8):
                    prev = hit
                    hit = q == jnp.asarray(j, bf16)
                    for k in range(2):
                        p0, p1, p2 = pieces[k]
                        cols[k].append(jnp.where(hit, p0, jnp.where(prev, p2, zb)))
                        cols[k].append(jnp.where(hit, p1, zb))
                spread.append([jnp.concatenate(c, 0) for c in cols])
            whi, wlo = [jnp.concatenate([spread[0][k], spread[1][k]], 1) for k in range(2)]
            two = nn(f_ref[...], whi)
            R = two[:256] + two[256:] + nn(f_ref[:256, :], wlo)
            for h in range(2):
                G = groups[h]
                V = R[:, 128 * h:128 * h + 128]
                d = sub_f - wide(G["start"], u)
                wb = [wide(w, u) for w in G["wb"]]
                c0 = pick_of([d == float(k) for k in range(3)], wb, z8)
                c1 = pick_of([d == float(k - 8) for k in (1, 2)], wb[1:], z8)
                q = wide(G["q"], u)
                bits = [(q & (1 << k)) != 0 for k in range(4)]

                def mux(v, b0, b1):
                    return jnp.where(b1, jnp.where(b0, v[3], v[2]), jnp.where(b0, v[1], v[0]))

                el, er, et, eb = [wide(e, u) for e in G["e"]]
                ga = [jnp.take_along_axis(tall, wide(t, u), axis=1) for t in G["ia"]]
                gb = [jnp.take_along_axis(flat, wide(t, u), axis=1) for t in G["ib"]]
                wh = [jnp.where(upper, wide(w[0], u), wide(w[1], u)) for w in G["w_half"]]
                beside = (wh[0] * ga[0] + wh[1] * ga[1] + wh[2] * ga[2]) * jnp.where(even, el, er)
                along = (wb[0] * gb[0] + wb[1] * gb[1] + wb[2] * gb[2] + el * west + er * east) * jnp.where(even, et, eb)
                for c in range(2):
                    r = [V[c * 128 + 8 * j:c * 128 + 8 * j + 8] for j in range(16)]
                    e = [mux([r[4 * m + t] for m in range(4)], bits[2], bits[3]) for t in range(4)]
                    e.append(mux([r[(4 * m + 4) % 16] for m in range(4)], bits[2], bits[3]))
                    first = mux(e[:4], bits[0], bits[1])
                    second = mux(e[1:], bits[0], bits[1])
                    total = first * c0 + second * c1 + jnp.where(own2[c], beside, 0.0) + jnp.where(own[c], along, 0.0)
                    row = PAD + 2 * (2 * u + h) + c
                    out_ref[pl.ds(i * (4 * S) + row, 1), :] = jnp.sum(total, axis=0, keepdims=True)
        return carry

    lax.fori_loop(0, OWNERS // S, step, 0)


def merge_kernel(d_ref, r1_ref, r2_ref, out_ref):
    S = out_ref.shape[1] // 256
    s0 = pl.program_id(0) * S
    sub = lax.broadcasted_iota(i32, (8, 128), 0)
    top, mid = sub < 2, sub < 4
    lead = pltpu.roll(r2_ref[0:8, :], 2, 0)
    for s in range(S):
        for h in range(2):
            src = s0 + s
            w = r1_ref[pl.ds(src * HEAD_ROWS + 2 * h, 8), :]
            at = src * BODY_ROWS + BODY * h - 2
            if s == 0 and h == 0:
                u = jnp.where(s0 == 0, lead, r2_ref[pl.ds(jnp.maximum(at, 0), 8), :])
            else:
                u = r2_ref[pl.ds(at, 8), :]
            d = d_ref[pl.ds(PAD + 2 * (2 * src + h) - 2, 8), :]
            out_ref[:, s * 256 + h * 128:s * 256 + h * 128 + 128] = jnp.where(top, w, jnp.where(mid, u + d, u))


def shape(*dims, dt=f32):
    return jax.ShapeDtypeStruct(dims, dt)


def held(*dims, dt=f32):
    return pltpu.VMEM(dims, dt)


def near_memory(x):
    return pltpu.with_memory_space_constraint(x, pltpu.VMEM)


def scratch(width):
    return [pltpu.VMEM((64 * width, 256), f32), pltpu.VMEM((128 * width + 16, PB), bf16), pltpu.VMEM((256, PB), bf16), pltpu.VMEM((8, 128), f32)]


def head(particles, key, a, b, velocity):
    n = particles.shape[1]
    return pl.pallas_call(
        head_kernel,
        out_shape=(held(OWNERS * HEAD_ROWS, 128), held(1, n), held(128, 128)),
        in_specs=[VMEM] * 5,
        out_specs=(VMEM,) * 3,
        scratch_shapes=scratch(HEAD) + [pltpu.VMEM((256, 256), bf16), pltpu.VMEM((RB // 2, 256), bf16)],
        name="head",
    )(particles, key, a, b, velocity)


def body(particles, key, rank, count, velocity):
    return pl.pallas_call(
        body_kernel,
        out_shape=(held(OWNERS * BODY_ROWS, 128), held(512, 256, dt=bf16)),
        in_specs=[VMEM] * 5,
        out_specs=(VMEM,) * 2,
        scratch_shapes=scratch(BODY),
        name="body",
    )(particles, key, near_memory(rank), near_memory(count), velocity)


def interp(arrived, fields):
    return pl.pallas_call(
        interp_kernel,
        out_shape=(held(PAD + 4 * OWNERS + 8, 128), shape(2 * OWNERS, 128, dt=i32)),
        in_specs=[VMEM] * 2,
        out_specs=(VMEM,) * 2,
        name="interp",
    )(arrived, near_memory(fields))


def merge(moved, head_arrived, body_arrived):
    n = OWNERS * 256
    g = 4
    return pl.pallas_call(
        merge_kernel,
        out_shape=shape(8, n),
        grid=(g,),
        in_specs=[VMEM] * 3,
        out_specs=pl.BlockSpec((8, n // g), lambda i: (0, i)),
        name="merge",
    )(near_memory(moved), head_arrived, body_arrived)


def exchange(buckets, rows):
    out = lax.all_to_all(buckets.reshape(OWNERS, rows, 1, 128), ALL, 0, 0, tiled=True)
    return near_memory(out.reshape(OWNERS * rows, 128))


def shards(particles, dest_key, cell_a, cell_b, velocity):
    key, a, b = [v.reshape(1, -1) for v in (dest_key, cell_a, cell_b)]
    first, rank, count = head(particles, key, a, b, velocity)
    arrived = exchange(first, HEAD_ROWS)
    second, fields = body(particles, key, rank, count, velocity)
    rest = exchange(second, BODY_ROWS)
    moved, cell = interp(arrived, fields)
    return merge(moved, arrived, rest), cell.reshape(-1)


def solution(mesh):
    split_mesh = Mesh(mesh.devices.reshape(mesh.shape["gx"], 4, 4, mesh.shape["gz"]), ALL)
    in_specs = (P(None, ALL), P(ALL), P(ALL), P(ALL), P(None, "gx", WIDE))
    out_specs = (P(None, ALL), P(ALL))
    return jax.shard_map(shards, mesh=split_mesh, in_specs=in_specs, out_specs=out_specs, check_vma=False)
```

```python
import jax
import jax.numpy as jnp
from jax import lax
from jax.experimental import pallas as pl
from jax.experimental.pallas import tpu as pltpu
from jax.sharding import Mesh
from jax.sharding import PartitionSpec as P

f32, bf16, i32 = jnp.float32, jnp.bfloat16, jnp.int32
ALL = ("gx", "gy_0", "gy_1", "gz")
WIDE = ("gy_0", "gy_1", "gz")
OWNERS = 128
HEAD = 3
BODY = 6
HEAD_ROWS = 8
BODY_ROWS = 12
HALO = 6
PAD = 8
RB = 4096
VMEM = pl.BlockSpec(memory_space=pltpu.VMEM)


def iota(shape, dim, dt):
    return lax.broadcasted_iota(i32, shape, dim).astype(f32).astype(dt)


def nt(a, b):
    return lax.dot_general(a, b, (((1,), (1,)), ((), ())), preferred_element_type=f32)


def nn(a, b):
    return jnp.dot(a, b, preferred_element_type=f32)


def split(v):
    hi = v.astype(bf16)
    return hi, (v - hi.astype(f32)).astype(bf16)


def one_hot(size, t):
    hit = iota((size, t.shape[1]), 0, bf16) == t.astype(bf16)
    return jnp.where(hit, jnp.ones((), bf16), jnp.zeros((), bf16))


def block(i, size):
    if isinstance(i, int):
        return slice(i * size, (i + 1) * size)
    return pl.ds(pl.multiple_of(i * size, size), size)


def column_of(key, rank, first):
    off = rank - first
    fits = (off >= 0.0) & (off < 128.0)
    return jnp.where(fits, off + jnp.where(key >= 64, 128.0, 0.0), -1.0)


def head_row(k, half):
    return 2 * half + k if k < 2 else 4 + half


def body_row(k, half):
    return BODY * half + k


def place_all(rows_of, width, row_at, stride, key_ref, rank_ref, counts, out_ref, acc_ref, left_ref, col_ref, hot_ref, more=None):
    size = left_ref.shape[1]
    n = key_ref.shape[1] // size
    m = 64 * width
    ids = lax.broadcasted_iota(i32, (128, 128), 0).astype(f32)
    n_full = jnp.sum(jnp.where(counts > 128.0, 1.0, 0.0), axis=0, keepdims=True)
    hot = jnp.max(jnp.where(counts > 128.0, ids, -1.0), axis=0, keepdims=True)
    lone = jnp.concatenate([jnp.where(n_full <= 1.0, hot, -1.0)] * (size // 128), 1)

    def fill(rows, low, t):
        pick = one_hot(64, low)
        for k, r in enumerate(rows):
            hi, lo = split(r)
            left_ref[k * 64:(k + 1) * 64, :] = pick * hi
            left_ref[m + k * 64:m + (k + 1) * 64, :] = pick * lo
        col_ref[...] = one_hot(256, t)

    def flush(half):
        for k in range(width):
            for o in range(2):
                at = pl.ds(o * 64 * stride + row_at(k, half), 64, stride=stride)
                out_ref[at, :] = acc_ref[k * 64:(k + 1) * 64, o * 128:(o + 1) * 128]

    for i in range(n):
        sl = block(i, size)
        key, rank = key_ref[0:1, sl], rank_ref[0:1, sl]
        rows = rows_of(sl)
        over = (key.astype(f32) == lone) & (rank >= 128.0)
        low = jnp.where(over, -1.0, (key & 63).astype(f32))
        fill(rows, low, jnp.where(over, rank - 128.0, column_of(key, rank, 0.0)))
        tail = jnp.concatenate([jnp.where(over, r, 0.0) for r in rows] + [jnp.zeros((8 - width, size), f32)], 0)
        hi = tail.astype(bf16).astype(f32)
        left_ref[2 * m:, :] = jnp.concatenate([hi, tail - hi], 0).astype(bf16)
        both = nt(left_ref[...], col_ref[...])
        placed = both[:m] + both[m:2 * m]
        spill = (both[2 * m:2 * m + 8] + both[2 * m + 8:])[:, :128]
        acc_ref[...] = acc_ref[...] + placed if i else placed
        hot_ref[...] = hot_ref[...] + spill if i else spill
    flush(0)
    base = jnp.max(jnp.maximum(hot, 0.0)).astype(i32) * stride
    for k in range(width):
        out_ref[pl.ds(base + row_at(k, 1), 1), :] = hot_ref[k:k + 1, :]
    if more:
        more()

    @pl.when(jnp.max(n_full) > 1.0)
    def _():
        acc_ref[...] = jnp.zeros(acc_ref.shape, f32)

        def again(i, carry):
            sl = block(i, size)
            key = key_ref[0:1, sl]
            fill(rows_of(sl), (key & 63).astype(f32), column_of(key, rank_ref[0:1, sl], 128.0))
            both = nt(left_ref[:2 * m, :], col_ref[...])
            acc_ref[...] += both[:m] + both[m:]
            return carry

        lax.fori_loop(0, n, again, 0)
        flush(1)


def around():
    x, y = lax.axis_index("gx"), lax.axis_index(WIDE)
    nx, ny = lax.axis_size("gx"), lax.axis_size(WIDE)

    def side(dx, dy):
        inside = (x + dx >= 0) & (x + dx < nx) & (y + dy >= 0) & (y + dy < ny)
        return inside, jnp.where(inside, (x + dx) * ny + y + dy, x * ny + y)

    return side


def head_kernel(p_ref, key_ref, a_ref, b_ref, v_ref, out_ref, rank_ref, count_ref, acc_ref, left_ref, col_ref, hot_ref, ut_ref, oh_ref, edge_ref, sem):
    n = p_ref.shape[1] // RB
    last = v_ref.shape[1] - 8
    copies = [pltpu.make_async_copy(v_ref.at[:, pl.ds(r, 8), :], edge_ref.at[e], sem.at[e]) for e, r in enumerate((0, last))]
    for copy in copies:
        copy.start()
    out_ref[...] = jnp.zeros(out_ref.shape, f32)
    before = lax.broadcasted_iota(i32, (256, 256), 0) < lax.broadcasted_iota(i32, (256, 256), 1)
    ut_ref[...] = jnp.where(before, 1.0, 0.0).astype(bf16)
    base = jnp.zeros((128, 1), f32)
    for i in range(n):
        key = key_ref[0:1, block(i, RB)].astype(f32)
        for k in range(RB // 256):
            oh_ref[k * 128:(k + 1) * 128, :] = one_hot(128, key[:, k * 256:(k + 1) * 256])
        res = nn(oh_ref[...], ut_ref[...])
        ranks = []
        for k in range(RB // 256):
            hot = oh_ref[k * 128:(k + 1) * 128, :]
            here = hot * (res[k * 128:(k + 1) * 128].astype(bf16) + base.astype(bf16))
            tree = [here[j * 16:(j + 1) * 16] for j in range(8)]
            while len(tree) > 1:
                tree = [u + v for u, v in zip(tree[::2], tree[1::2])]
            ranks.append(jnp.sum(tree[0].astype(f32), axis=0, keepdims=True))
            pair = (hot[:, :128] + hot[:, 128:]).astype(f32)
            base = base + jnp.sum(pair, axis=1, keepdims=True)
        rank_ref[0:1, block(i, RB)] = jnp.concatenate(ranks, 1)
    count_ref[...] = jnp.broadcast_to(base, (128, 128))
    for copy in copies:
        copy.wait()
    side = around()

    def rows_of(sl):
        cell = (a_ref[0:1, sl] * 128 + b_ref[0:1, sl] + 1).astype(f32)
        return [p_ref[0:1, sl], p_ref[1:2, sl], cell]

    def halo():
        for e, dx in enumerate((-1, 1)):
            for dy in (-1, 0, 1):
                at = side(dx, dy)[1] * HEAD_ROWS + HALO
                for c in range(2):
                    row = 7 if e else 0
                    out_ref[pl.ds(at + c, 1), :] = edge_ref[e, c, row:row + 1, :]

    place_all(rows_of, HEAD, head_row, HEAD_ROWS, key_ref, rank_ref, count_ref[...], out_ref, acc_ref, left_ref, col_ref, hot_ref, halo)


def body_kernel(p_ref, key_ref, rank_ref, count_ref, v_ref, out_ref, f_ref, first_ref, last_ref, acc_ref, left_ref, col_ref, hot_ref):
    out_ref[...] = jnp.zeros(out_ref.shape, f32)
    for c in range(2):
        turned = v_ref[c].T
        first_ref[c:c + 1, :] = turned[0:1]
        last_ref[c:c + 1, :] = turned[127:128]
        hi, lo = split(turned)
        f_ref[c * 128:(c + 1) * 128, :] = hi
        f_ref[256 + c * 128:256 + (c + 1) * 128, :] = lo

    def rows_of(sl):
        return [p_ref[k:k + 1, sl] for k in range(2, 8)]

    place_all(rows_of, BODY, body_row, BODY_ROWS, key_ref, rank_ref, count_ref[...], out_ref, acc_ref, left_ref, col_ref, hot_ref)


def quad(t):
    return 0.5 * t * (t - 1.0), 1.0 - t * t, 0.5 * t * (t + 1.0)


def pick_of(hits, values, zero):
    out = zero
    for h, v in reversed(list(zip(hits, values))):
        out = jnp.where(h, v, out)
    return out


def interp_kernel(r_ref, f_ref, tall_ref, out_ref, cell_ref):
    S = 16
    side = around()

    def from_side(dx, dy, k):
        inside, who = side(dx, dy)
        row = r_ref[pl.ds(who * HEAD_ROWS + HALO + k, 1), :]
        return jnp.where(inside, row, 0.0)

    z4 = jnp.zeros((4, 128), f32)
    flat = jnp.concatenate([from_side(dx, 0, c) for c in range(2) for dx in (-1, 1)] + [z4], 0)
    west = jnp.concatenate([from_side(dx, -1, c) for c in range(2) for dx in (-1, 1)] + [z4], 0)
    east = jnp.concatenate([from_side(dx, 1, c) for c in range(2) for dx in (-1, 1)] + [z4], 0)
    west = jnp.broadcast_to(west[:, 127:128], (8, 128))
    east = jnp.broadcast_to(east[:, 0:1], (8, 128))
    tall = tall_ref[...]
    sub = lax.broadcasted_iota(i32, (8, 128), 0)
    even = (sub & 1) == 0
    upper = sub < 4
    own = [(sub >> 1) == c for c in range(2)]
    own2 = [((sub >> 1) & 1) == c for c in range(2)]
    sub_f = sub.astype(f32)
    row_b = iota((16, 128), 0, bf16)
    zb = jnp.zeros((16, 128), bf16)
    z8 = jnp.zeros((8, 128), f32)

    def step(i, carry):
        groups = []
        for h in range(2):
            f, g, cell = [r_ref[pl.ds(i * (S * HEAD_ROWS) + head_row(k, h), S, stride=HEAD_ROWS), :] for k in range(3)]
            ci = cell.astype(i32) - 1
            cell_ref[pl.ds(i * (2 * S) + h, S, stride=2), :] = ci
            live = ci >= 0
            a = jnp.where(live, ci >> 7, 0)
            b = ci & 127
            half = jnp.where(live, 0.5, 0.0)
            wa = [half * w for w in quad(f)]
            wb = list(quad(g))
            hi = [w.astype(bf16).astype(f32) for w in wa]
            lo = [w - v for w, v in zip(wa, hi)]
            el, er = jnp.where(b == 0, wb[0], 0.0), jnp.where(b == 127, wb[2], 0.0)
            wb[0], wb[2] = wb[0] - el, wb[2] - er
            et, eb = jnp.where(a == 0, wa[0], 0.0), jnp.where(a == 255, wa[2], 0.0)
            at_a = [a - 1 + k for k in range(3)]
            w_half = [[jnp.where((t >> 7) == k, w, 0.0) for k in range(2)] for t, w in zip(at_a, wa)]
            groups.append(dict(
                w=hi + lo + [((a - 1) & 31).astype(f32), ((a - 1) >> 5).astype(f32)],
                wb=wb, start=((b - 1) & 7).astype(f32), q=((b - 1) >> 3) & 15, e=[el, er, et, eb],
                ia=[t & 127 for t in at_a], ib=[(b - 1 + k) & 127 for k in range(3)], w_half=w_half))

        def wide(x, j):
            return jnp.broadcast_to(x[j:j + 1], (8, 128))

        for u in range(S):
            spread = []
            for h in range(2):
                G = groups[h]
                packed = []
                for x in G["w"]:
                    y = wide(x, u)
                    packed.append(jnp.concatenate([y, y], 0).astype(bf16))
                his, los, start, q = packed[:3], packed[3:6], packed[6], packed[7]
                d = row_b - start
                near = [d == jnp.asarray(k, bf16) for k in range(3)]
                far = [d == jnp.asarray(k - 16, bf16) for k in range(3)]
                over = [d == jnp.asarray(k - 32, bf16) for k in (1, 2)]
                pieces = []
                for w in (his, los):
                    pieces.append((pick_of(near, w, zb), pick_of(far, w, zb), pick_of(over, w[1:], zb)))
                hit = q == jnp.asarray(-1, bf16)
                cols = [[], []]
                for j in range(8):
                    prev = hit
                    hit = q == jnp.asarray(j, bf16)
                    for k in range(2):
                        p0, p1, p2 = pieces[k]
                        cols[k].append(jnp.where(hit, p0, jnp.where(prev, p2, zb)))
                        cols[k].append(jnp.where(hit, p1, zb))
                spread.append([jnp.concatenate(c, 0) for c in cols])
            whi, wlo = [jnp.concatenate([spread[0][k], spread[1][k]], 1) for k in range(2)]
            two = nn(f_ref[...], whi)
            R = two[:256] + two[256:] + nn(f_ref[:256, :], wlo)
            for h in range(2):
                G = groups[h]
                V = R[:, 128 * h:128 * h + 128]
                d = sub_f - wide(G["start"], u)
                wb = [wide(w, u) for w in G["wb"]]
                c0 = pick_of([d == float(k) for k in range(3)], wb, z8)
                c1 = pick_of([d == float(k - 8) for k in (1, 2)], wb[1:], z8)
                q = wide(G["q"], u)
                bits = [(q & (1 << k)) != 0 for k in range(4)]

                def mux(v, b0, b1):
                    return jnp.where(b1, jnp.where(b0, v[3], v[2]), jnp.where(b0, v[1], v[0]))

                el, er, et, eb = [wide(e, u) for e in G["e"]]
                ga = [jnp.take_along_axis(tall, wide(t, u), axis=1) for t in G["ia"]]
                gb = [jnp.take_along_axis(flat, wide(t, u), axis=1) for t in G["ib"]]
                wh = [jnp.where(upper, wide(w[0], u), wide(w[1], u)) for w in G["w_half"]]
                beside = (wh[0] * ga[0] + wh[1] * ga[1] + wh[2] * ga[2]) * jnp.where(even, el, er)
                along = (wb[0] * gb[0] + wb[1] * gb[1] + wb[2] * gb[2] + el * west + er * east) * jnp.where(even, et, eb)
                for c in range(2):
                    r = [V[c * 128 + 8 * j:c * 128 + 8 * j + 8] for j in range(16)]
                    e = [mux([r[4 * m + t] for m in range(4)], bits[2], bits[3]) for t in range(4)]
                    e.append(mux([r[(4 * m + 4) % 16] for m in range(4)], bits[2], bits[3]))
                    first = mux(e[:4], bits[0], bits[1])
                    second = mux(e[1:], bits[0], bits[1])
                    total = first * c0 + second * c1 + jnp.where(own2[c], beside, 0.0) + jnp.where(own[c], along, 0.0)
                    row = PAD + 2 * (2 * u + h) + c
                    out_ref[pl.ds(i * (4 * S) + row, 1), :] = jnp.sum(total, axis=0, keepdims=True)
        return carry

    lax.fori_loop(0, OWNERS // S, step, 0)


def merge_kernel(d_ref, r1_ref, r2_ref, out_ref):
    S = out_ref.shape[1] // 256
    s0 = pl.program_id(0) * S
    sub = lax.broadcasted_iota(i32, (8, 128), 0)
    top, mid = sub < 2, sub < 4
    lead = pltpu.roll(r2_ref[0:8, :], 2, 0)
    for s in range(S):
        for h in range(2):
            src = s0 + s
            w = r1_ref[pl.ds(pl.multiple_of(src * HEAD_ROWS, HEAD_ROWS), 8), :]
            w = pltpu.roll(w, 6, 0) if h else w
            at = src * BODY_ROWS + BODY * h - 2
            if s == 0 and h == 0:
                u = jnp.where(s0 == 0, lead, r2_ref[pl.ds(jnp.maximum(at, 0), 8), :])
            else:
                u = r2_ref[pl.ds(at, 8), :]
            d = d_ref[pl.ds(PAD + 2 * (2 * src + h) - 2, 8), :]
            out_ref[:, s * 256 + h * 128:s * 256 + h * 128 + 128] = jnp.where(top, w, jnp.where(mid, u + d, u))


def shape(*dims, dt=f32):
    return jax.ShapeDtypeStruct(dims, dt)


def held(*dims, dt=f32):
    return pltpu.VMEM(dims, dt)


def near_memory(x):
    return pltpu.with_memory_space_constraint(x, pltpu.VMEM)


def scratch(width, size):
    return [pltpu.VMEM((64 * width, 256), f32), pltpu.VMEM((128 * width + 16, size), bf16), pltpu.VMEM((256, size), bf16), pltpu.VMEM((8, 128), f32)]


def head(particles, key, a, b, velocity):
    n = particles.shape[1]
    return pl.pallas_call(
        head_kernel,
        out_shape=(held(OWNERS * HEAD_ROWS, 128), held(1, n), held(128, 128)),
        in_specs=[VMEM] * 4 + [pl.BlockSpec(memory_space=pl.ANY)],
        out_specs=(VMEM,) * 3,
        scratch_shapes=scratch(HEAD, n // 2)
        + [pltpu.VMEM((256, 256), bf16), pltpu.VMEM((RB // 2, 256), bf16), pltpu.VMEM((2, 2, 8, 128), f32), pltpu.SemaphoreType.DMA((2,))],
        name="head",
    )(particles, key, a, b, velocity)


def body(particles, key, rank, count, velocity):
    return pl.pallas_call(
        body_kernel,
        out_shape=(held(OWNERS * BODY_ROWS, 128), held(512, 256, dt=bf16), shape(2, 256), shape(2, 256)),
        in_specs=[VMEM] * 5,
        out_specs=(VMEM,) * 4,
        scratch_shapes=scratch(BODY, particles.shape[1]),
        name="body",
    )(particles, key, near_memory(rank), near_memory(count), velocity)


def tall_kernel(west_ref, east_ref, out_ref):
    for h in range(2):
        for c in range(2):
            for k, ref in enumerate((west_ref, east_ref)):
                out_ref[4 * h + 2 * c + k:4 * h + 2 * c + k + 1, :] = ref[c:c + 1, h * 128:(h + 1) * 128]


def tall_sides(west, east):
    return pl.pallas_call(tall_kernel, out_shape=held(8, 128), in_specs=[VMEM] * 2, out_specs=VMEM, name="tall")(near_memory(west), near_memory(east))


def interp(arrived, fields, tall):
    return pl.pallas_call(
        interp_kernel,
        out_shape=(held(PAD + 4 * OWNERS + 8, 128), shape(2 * OWNERS, 128, dt=i32)),
        in_specs=[VMEM] * 3,
        out_specs=(VMEM,) * 2,
        name="interp",
    )(arrived, near_memory(fields), near_memory(tall))


def merge(moved, head_arrived, body_arrived):
    n = OWNERS * 256
    g = 4
    return pl.pallas_call(
        merge_kernel,
        out_shape=shape(8, n),
        grid=(g,),
        in_specs=[VMEM] * 3,
        out_specs=pl.BlockSpec((8, n // g), lambda i: (0, i)),
        name="merge",
    )(near_memory(moved), head_arrived, body_arrived)


def both_sides(first, last, axis):
    peers = lax.axis_size(axis)
    up = [(i, i + 1) for i in range(peers - 1)]
    down = [(j, i) for i, j in up]
    return lax.ppermute(last, axis, up), lax.ppermute(first, axis, down)


def exchange(buckets, rows):
    out = lax.all_to_all(buckets.reshape(OWNERS, rows, 1, 128), ALL, 0, 0, tiled=True)
    return near_memory(out.reshape(OWNERS * rows, 128))


def shards(particles, dest_key, cell_a, cell_b, velocity):
    key, a, b = [v.reshape(1, -1) for v in (dest_key, cell_a, cell_b)]
    near, rank, count = head(particles, key, a, b, velocity)
    arrived = exchange(near, HEAD_ROWS)
    far, fields, first, last = body(particles, key, rank, count, velocity)
    tall = tall_sides(*both_sides(first, last, WIDE))
    rest = exchange(far, BODY_ROWS)
    moved, cell = interp(arrived, fields, tall)
    return merge(moved, arrived, rest), cell.reshape(-1)


def solution(mesh):
    split_mesh = Mesh(mesh.devices.reshape(mesh.shape["gx"], 4, 4, mesh.shape["gz"]), ALL)
    in_specs = (P(None, ALL), P(ALL), P(ALL), P(ALL), P(None, "gx", WIDE))
    out_specs = (P(None, ALL), P(ALL))
    return jax.shard_map(shards, mesh=split_mesh, in_specs=in_specs, out_specs=out_specs, check_vma=False)
```

```python
import jax
import jax.numpy as jnp
from jax import lax
from jax.experimental import pallas as pl
from jax.experimental.pallas import tpu as pltpu
from jax.sharding import Mesh
from jax.sharding import PartitionSpec as P

f32, bf16, i32 = jnp.float32, jnp.bfloat16, jnp.int32
ALL = ("gx", "gy_0", "gy_1", "gz")
WIDE = ("gy_0", "gy_1", "gz")
OWNERS = 128
HEAD = 3
BODY = 6
HEAD_ROWS = 10
BODY_ROWS = 12
HALO = 6
PAD = 8
RB = 4096
VMEM = pl.BlockSpec(memory_space=pltpu.VMEM)


def iota(shape, dim, dt):
    return lax.broadcasted_iota(i32, shape, dim).astype(f32).astype(dt)


def nt(a, b):
    return lax.dot_general(a, b, (((1,), (1,)), ((), ())), preferred_element_type=f32)


def nn(a, b):
    return jnp.dot(a, b, preferred_element_type=f32)


def split(v):
    hi = v.astype(bf16)
    return hi, (v - hi.astype(f32)).astype(bf16)


def one_hot(size, t):
    hit = iota((size, t.shape[1]), 0, bf16) == t.astype(bf16)
    return jnp.where(hit, jnp.ones((), bf16), jnp.zeros((), bf16))


def block(i, size):
    if isinstance(i, int):
        return slice(i * size, (i + 1) * size)
    return pl.ds(pl.multiple_of(i * size, size), size)


def column_of(key, rank, first):
    off = rank - first
    fits = (off >= 0.0) & (off < 128.0)
    return jnp.where(fits, off + jnp.where(key >= 64, 128.0, 0.0), -1.0)


def head_row(k, half):
    return 2 * half + k if k < 2 else 4 + half


def body_row(k, half):
    return BODY * half + k


def place_all(rows_of, width, row_at, stride, key_ref, rank_ref, counts, out_ref, acc_ref, left_ref, col_ref, more=None):
    size = left_ref.shape[1]
    n = key_ref.shape[1] // size
    m = 64 * width
    ids = lax.broadcasted_iota(i32, (128, 128), 0).astype(f32)
    n_full = jnp.sum(jnp.where(counts > 128.0, 1.0, 0.0), axis=0, keepdims=True)
    hot = jnp.max(jnp.where(counts > 128.0, ids, -1.0), axis=0, keepdims=True)
    lone = jnp.concatenate([jnp.where(n_full <= 1.0, hot, -1.0)] * (size // 128), 1)

    def fill(rows, low, t):
        pick = one_hot(64, low)
        for k, r in enumerate(rows):
            hi, lo = split(r)
            left_ref[k * 64:(k + 1) * 64, :] = pick * hi
            left_ref[m + k * 64:m + (k + 1) * 64, :] = pick * lo
        col_ref[...] = one_hot(256, t)

    def flush(half, terms):
        for k in range(width):
            for o in range(2):
                at = pl.ds(o * 64 * stride + row_at(k, half), 64, stride=stride)
                lanes = slice(o * 128, (o + 1) * 128)
                out_ref[at, :] = sum(acc_ref[t, r + k * 64:r + (k + 1) * 64, lanes] for t, r in terms)

    for i in range(n):
        sl = block(i, size)
        key, rank = key_ref[0:1, sl], rank_ref[0:1, sl]
        rows = rows_of(sl)
        over = (key.astype(f32) == lone) & (rank >= 128.0)
        low = jnp.where(over, -1.0, (key & 63).astype(f32))
        fill(rows, low, jnp.where(over, rank - 128.0, column_of(key, rank, 0.0)))
        tail = jnp.concatenate([jnp.where(over, r, 0.0) for r in rows] + [jnp.zeros((8 - width, size), f32)], 0)
        hi = tail.astype(bf16).astype(f32)
        left_ref[2 * m:, :] = jnp.concatenate([hi, tail - hi], 0).astype(bf16)
        for k in range(2):
            lanes = slice(k * size // 2, (k + 1) * size // 2)
            acc_ref[2 * i + k] = nt(left_ref[:, lanes], col_ref[:, lanes])
    flush(0, [(k, part * m) for k in range(2 * n) for part in range(2)])
    spill = sum(acc_ref[k, 2 * m + 8 * j:2 * m + 8 * j + 8, :128] for k in range(2 * n) for j in range(2))
    base = jnp.max(jnp.maximum(hot, 0.0)).astype(i32) * stride
    for k in range(width):
        out_ref[pl.ds(base + row_at(k, 1), 1), :] = spill[k:k + 1]
    if more:
        more()

    @pl.when(jnp.max(n_full) > 1.0)
    def _():
        acc_ref[0] = jnp.zeros(acc_ref.shape[1:], f32)

        def again(i, carry):
            sl = block(i, size)
            key = key_ref[0:1, sl]
            fill(rows_of(sl), (key & 63).astype(f32), column_of(key, rank_ref[0:1, sl], 128.0))
            acc_ref[0, :2 * m, :] += nt(left_ref[:2 * m, :], col_ref[...])
            return carry

        lax.fori_loop(0, n, again, 0)
        flush(1, [(0, 0), (0, m)])


def around():
    x, y = lax.axis_index("gx"), lax.axis_index(WIDE)
    nx, ny = lax.axis_size("gx"), lax.axis_size(WIDE)

    def side(dx, dy):
        inside = (x + dx >= 0) & (x + dx < nx) & (y + dy >= 0) & (y + dy < ny)
        return inside, jnp.where(inside, (x + dx) * ny + y + dy, x * ny + y)

    return side


def head_kernel(p_ref, key_ref, a_ref, b_ref, v_ref, out_ref, rank_ref, count_ref, acc_ref, left_ref, col_ref, ut_ref, oh_ref, edge_ref, sem):
    n = p_ref.shape[1] // RB
    copy = pltpu.make_async_copy(v_ref, edge_ref, sem)
    copy.start()
    out_ref[...] = jnp.zeros(out_ref.shape, f32)
    before = lax.broadcasted_iota(i32, (256, 256), 0) < lax.broadcasted_iota(i32, (256, 256), 1)
    ut_ref[...] = jnp.where(before, 1.0, 0.0).astype(bf16)
    count_ref[...] = jnp.zeros(count_ref.shape, f32)

    def rank_block(i, carry):
        sl = block(i, RB)
        key = key_ref[0:1, sl].astype(f32)
        for k in range(RB // 256):
            oh_ref[k * 128:(k + 1) * 128, :] = one_hot(128, key[:, k * 256:(k + 1) * 256])
        res = nn(oh_ref[...], ut_ref[...])
        base = count_ref[...]
        ranks = []
        for k in range(RB // 256):
            hot = oh_ref[k * 128:(k + 1) * 128, :]
            low = base.astype(bf16)
            here = hot * (res[k * 128:(k + 1) * 128].astype(bf16) + jnp.concatenate([low, low], 1))
            tree = [here[j * 16:(j + 1) * 16] for j in range(8)]
            while len(tree) > 1:
                tree = [u + v for u, v in zip(tree[::2], tree[1::2])]
            ranks.append(jnp.sum(tree[0].astype(f32), axis=0, keepdims=True))
            pair = (hot[:, :128] + hot[:, 128:]).astype(f32)
            base = base + jnp.sum(pair, axis=1, keepdims=True)
        count_ref[...] = base
        rank_ref[0:1, sl] = jnp.concatenate(ranks, 1)
        return carry

    lax.fori_loop(0, n, rank_block, 0)
    copy.wait()
    side = around()
    turned = [edge_ref[c].T for c in range(2)]

    def rows_of(sl):
        cell = (a_ref[0:1, sl] * 128 + b_ref[0:1, sl] + 1).astype(f32)
        return [p_ref[0:1, sl], p_ref[1:2, sl], cell]

    def halo():
        for dx in (-1, 0, 1):
            for dy in (-1, 0, 1):
                at = side(dx, dy)[1] * HEAD_ROWS + HALO
                for c in range(2):
                    if dx:
                        row = edge_ref.shape[1] - 1 if dx > 0 else 0
                        out_ref[pl.ds(at + c, 1), :] = edge_ref[c, row:row + 1, :]
                    elif dy:
                        col = edge_ref.shape[2] - 1 if dy > 0 else 0
                        for h in range(2):
                            out_ref[pl.ds(at + 2 * c + h, 1), :] = turned[c][col:col + 1, h * 128:(h + 1) * 128]

    place_all(rows_of, HEAD, head_row, HEAD_ROWS, key_ref, rank_ref, count_ref[...], out_ref, acc_ref, left_ref, col_ref, halo)


def body_kernel(p_ref, key_ref, rank_ref, count_ref, v_ref, out_ref, f_ref, acc_ref, left_ref, col_ref):
    out_ref[...] = jnp.zeros(out_ref.shape, f32)
    for c in range(2):
        hi, lo = split(v_ref[c].T)
        f_ref[c * 128:(c + 1) * 128, :] = hi
        f_ref[256 + c * 128:256 + (c + 1) * 128, :] = lo

    def rows_of(sl):
        return [p_ref[k:k + 1, sl] for k in range(2, 8)]

    place_all(rows_of, BODY, body_row, BODY_ROWS, key_ref, rank_ref, count_ref[...], out_ref, acc_ref, left_ref, col_ref)


def quad(t):
    return 0.5 * t * (t - 1.0), 1.0 - t * t, 0.5 * t * (t + 1.0)


def pick_of(hits, values, zero):
    out = zero
    for h, v in reversed(list(zip(hits, values))):
        out = jnp.where(h, v, out)
    return out


def interp_kernel(r_ref, f_ref, out_ref, cell_ref):
    S = 16
    side = around()

    def from_side(dx, dy, k):
        inside, who = side(dx, dy)
        row = r_ref[pl.ds(who * HEAD_ROWS + HALO + k, 1), :]
        return jnp.where(inside, row, 0.0)

    z4 = jnp.zeros((4, 128), f32)
    flat = jnp.concatenate([from_side(dx, 0, c) for c in range(2) for dx in (-1, 1)] + [z4], 0)
    west = jnp.concatenate([from_side(dx, -1, c) for c in range(2) for dx in (-1, 1)] + [z4], 0)
    east = jnp.concatenate([from_side(dx, 1, c) for c in range(2) for dx in (-1, 1)] + [z4], 0)
    west = jnp.broadcast_to(west[:, 127:128], (8, 128))
    east = jnp.broadcast_to(east[:, 0:1], (8, 128))
    tall = jnp.concatenate([from_side(0, dy, 2 * c + h) for h in range(2) for c in range(2) for dy in (-1, 1)], 0)
    sub = lax.broadcasted_iota(i32, (8, 128), 0)
    even = (sub & 1) == 0
    upper = sub < 4
    own = [(sub >> 1) == c for c in range(2)]
    own2 = [((sub >> 1) & 1) == c for c in range(2)]
    sub_f = sub.astype(f32)
    row_b = iota((16, 128), 0, bf16)
    zb = jnp.zeros((16, 128), bf16)
    z8 = jnp.zeros((8, 128), f32)

    def step(i, carry):
        groups = []
        for h in range(2):
            f, g, cell = [r_ref[pl.ds(i * (S * HEAD_ROWS) + head_row(k, h), S, stride=HEAD_ROWS), :] for k in range(3)]
            ci = cell.astype(i32) - 1
            cell_ref[pl.ds(i * (2 * S) + h, S, stride=2), :] = ci
            live = ci >= 0
            a = jnp.where(live, ci >> 7, 0)
            b = ci & 127
            half = jnp.where(live, 0.5, 0.0)
            wa = [half * w for w in quad(f)]
            wb = list(quad(g))
            hi = [w.astype(bf16).astype(f32) for w in wa]
            lo = [w - v for w, v in zip(wa, hi)]
            el, er = jnp.where(b == 0, wb[0], 0.0), jnp.where(b == 127, wb[2], 0.0)
            wb[0], wb[2] = wb[0] - el, wb[2] - er
            et, eb = jnp.where(a == 0, wa[0], 0.0), jnp.where(a == 255, wa[2], 0.0)
            at_a = [a - 1 + k for k in range(3)]
            w_half = [[jnp.where((t >> 7) == k, w, 0.0) for k in range(2)] for t, w in zip(at_a, wa)]
            groups.append(dict(
                w=hi + lo + [((a - 1) & 31).astype(f32), ((a - 1) >> 5).astype(f32)],
                wb=wb, start=((b - 1) & 7).astype(f32), q=((b - 1) >> 3) & 15, e=[el, er, et, eb],
                ia=[t & 127 for t in at_a], ib=[(b - 1 + k) & 127 for k in range(3)], w_half=w_half))

        def wide(x, j):
            return jnp.broadcast_to(x[j:j + 1], (8, 128))

        for u in range(S):
            spread = []
            for h in range(2):
                G = groups[h]
                packed = []
                for x in G["w"]:
                    y = wide(x, u)
                    packed.append(jnp.concatenate([y, y], 0).astype(bf16))
                his, los, start, q = packed[:3], packed[3:6], packed[6], packed[7]
                d = row_b - start
                near = [d == jnp.asarray(k, bf16) for k in range(3)]
                far = [d == jnp.asarray(k - 16, bf16) for k in range(3)]
                over = [d == jnp.asarray(k - 32, bf16) for k in (1, 2)]
                pieces = []
                for w in (his, los):
                    pieces.append((pick_of(near, w, zb), pick_of(far, w, zb), pick_of(over, w[1:], zb)))
                hit = q == jnp.asarray(-1, bf16)
                cols = [[], []]
                for j in range(8):
                    prev = hit
                    hit = q == jnp.asarray(j, bf16)
                    for k in range(2):
                        p0, p1, p2 = pieces[k]
                        cols[k].append(jnp.where(hit, p0, jnp.where(prev, p2, zb)))
                        cols[k].append(jnp.where(hit, p1, zb))
                spread.append([jnp.concatenate(c, 0) for c in cols])
            whi, wlo = [jnp.concatenate([spread[0][k], spread[1][k]], 1) for k in range(2)]
            two = nn(f_ref[...], whi)
            R = two[:256] + two[256:] + nn(f_ref[:256, :], wlo)
            for h in range(2):
                G = groups[h]
                V = R[:, 128 * h:128 * h + 128]
                d = sub_f - wide(G["start"], u)
                wb = [wide(w, u) for w in G["wb"]]
                c0 = pick_of([d == float(k) for k in range(3)], wb, z8)
                c1 = pick_of([d == float(k - 8) for k in (1, 2)], wb[1:], z8)
                q = wide(G["q"], u)
                bits = [(q & (1 << k)) != 0 for k in range(4)]

                def mux(v, b0, b1):
                    return jnp.where(b1, jnp.where(b0, v[3], v[2]), jnp.where(b0, v[1], v[0]))

                el, er, et, eb = [wide(e, u) for e in G["e"]]
                ga = [jnp.take_along_axis(tall, wide(t, u), axis=1) for t in G["ia"]]
                gb = [jnp.take_along_axis(flat, wide(t, u), axis=1) for t in G["ib"]]
                wh = [jnp.where(upper, wide(w[0], u), wide(w[1], u)) for w in G["w_half"]]
                beside = (wh[0] * ga[0] + wh[1] * ga[1] + wh[2] * ga[2]) * jnp.where(even, el, er)
                along = (wb[0] * gb[0] + wb[1] * gb[1] + wb[2] * gb[2] + el * west + er * east) * jnp.where(even, et, eb)
                for c in range(2):
                    r = [V[c * 128 + 8 * j:c * 128 + 8 * j + 8] for j in range(16)]
                    e = [mux([r[4 * m + t] for m in range(4)], bits[2], bits[3]) for t in range(4)]
                    e.append(mux([r[(4 * m + 4) % 16] for m in range(4)], bits[2], bits[3]))
                    first = mux(e[:4], bits[0], bits[1])
                    second = mux(e[1:], bits[0], bits[1])
                    total = first * c0 + second * c1 + jnp.where(own2[c], beside, 0.0) + jnp.where(own[c], along, 0.0)
                    row = PAD + 2 * (2 * u + h) + c
                    out_ref[pl.ds(i * (4 * S) + row, 1), :] = jnp.sum(total, axis=0, keepdims=True)
        return carry

    lax.fori_loop(0, OWNERS // S, step, 0)


def merge_kernel(d_ref, r1_ref, r2_ref, out_ref):
    S = out_ref.shape[1] // 256
    s0 = pl.program_id(0) * S
    sub = lax.broadcasted_iota(i32, (8, 128), 0)
    top, mid = sub < 2, sub < 4
    lead = pltpu.roll(r2_ref[0:8, :], 2, 0)
    for s in range(S):
        for h in range(2):
            src = s0 + s
            w = r1_ref[pl.ds(src * HEAD_ROWS + 2 * h, 8), :]
            at = src * BODY_ROWS + BODY * h - 2
            if s == 0 and h == 0:
                u = jnp.where(s0 == 0, lead, r2_ref[pl.ds(jnp.maximum(at, 0), 8), :])
            else:
                u = r2_ref[pl.ds(at, 8), :]
            d = d_ref[pl.ds(PAD + 2 * (2 * src + h) - 2, 8), :]
            out_ref[:, s * 256 + h * 128:s * 256 + h * 128 + 128] = jnp.where(top, w, jnp.where(mid, u + d, u))


def shape(*dims, dt=f32):
    return jax.ShapeDtypeStruct(dims, dt)


def held(*dims, dt=f32):
    return pltpu.VMEM(dims, dt)


def near_memory(x):
    return pltpu.with_memory_space_constraint(x, pltpu.VMEM)


def scratch(width, size):
    rows = 128 * width + 16
    return [pltpu.VMEM((16384 // size, rows, 256), f32), pltpu.VMEM((rows, size), bf16), pltpu.VMEM((256, size), bf16)]


def head(particles, key, a, b, velocity):
    n = particles.shape[1]
    return pl.pallas_call(
        head_kernel,
        out_shape=(held(OWNERS * HEAD_ROWS, 128), held(1, n), held(128, 128)),
        in_specs=[VMEM] * 4 + [pl.BlockSpec(memory_space=pl.ANY)],
        out_specs=(VMEM,) * 3,
        scratch_shapes=scratch(HEAD, n // 2)
        + [pltpu.VMEM((256, 256), bf16), pltpu.VMEM((RB // 2, 256), bf16), pltpu.VMEM((2, 256, 128), f32), pltpu.SemaphoreType.DMA],
        name="head",
    )(particles, key, a, b, velocity)


def body(particles, key, rank, count, velocity):
    return pl.pallas_call(
        body_kernel,
        out_shape=(held(OWNERS * BODY_ROWS, 128), held(512, 256, dt=bf16)),
        in_specs=[VMEM] * 5,
        out_specs=(VMEM,) * 2,
        scratch_shapes=scratch(BODY, particles.shape[1] // 2),
        name="body",
    )(particles, key, near_memory(rank), near_memory(count), velocity)


def interp(arrived, fields):
    return pl.pallas_call(
        interp_kernel,
        out_shape=(held(PAD + 4 * OWNERS + 8, 128), shape(2 * OWNERS, 128, dt=i32)),
        in_specs=[VMEM] * 2,
        out_specs=(VMEM,) * 2,
        name="interp",
    )(arrived, near_memory(fields))


def merge(moved, head_arrived, body_arrived):
    n = OWNERS * 256
    g = 4
    return pl.pallas_call(
        merge_kernel,
        out_shape=shape(8, n),
        grid=(g,),
        in_specs=[VMEM] * 3,
        out_specs=pl.BlockSpec((8, n // g), lambda i: (0, i)),
        name="merge",
    )(near_memory(moved), head_arrived, body_arrived)


def exchange(buckets, rows):
    out = lax.all_to_all(buckets.reshape(OWNERS, rows, 1, 128), ALL, 0, 0, tiled=True)
    return near_memory(out.reshape(OWNERS * rows, 128))


def shards(particles, dest_key, cell_a, cell_b, velocity):
    key, a, b = [v.reshape(1, -1) for v in (dest_key, cell_a, cell_b)]
    first, rank, count = head(particles, key, a, b, velocity)
    arrived = exchange(first, HEAD_ROWS)
    second, fields = body(particles, key, rank, count, velocity)
    rest = exchange(second, BODY_ROWS)
    moved, cell = interp(arrived, fields)
    return merge(moved, arrived, rest), cell.reshape(-1)


def solution(mesh):
    split_mesh = Mesh(mesh.devices.reshape(mesh.shape["gx"], 4, 4, mesh.shape["gz"]), ALL)
    in_specs = (P(None, ALL), P(ALL), P(ALL), P(ALL), P(None, "gx", WIDE))
    out_specs = (P(None, ALL), P(ALL))
    return jax.shard_map(shards, mesh=split_mesh, in_specs=in_specs, out_specs=out_specs, check_vma=False)
```

```python
import jax
import jax.numpy as jnp
from jax import lax
from jax.experimental import pallas as pl
from jax.experimental.pallas import tpu as pltpu
from jax.sharding import Mesh
from jax.sharding import PartitionSpec as P

f32, bf16, i32 = jnp.float32, jnp.bfloat16, jnp.int32
ALL = ("gx", "gy_0", "gy_1", "gz")
WIDE = ("gy_0", "gy_1", "gz")
OWNERS = 128
HEAD = 3
BODY = 6
HEAD_ROWS = 10
BODY_ROWS = 12
HALO = 6
PAD = 8
RB = 4096
MERGES = 4
VMEM = pl.BlockSpec(memory_space=pltpu.VMEM)


def iota(shape, dim, dt):
    return lax.broadcasted_iota(i32, shape, dim).astype(f32).astype(dt)


def nt(a, b):
    return lax.dot_general(a, b, (((1,), (1,)), ((), ())), preferred_element_type=f32)


def nn(a, b):
    return jnp.dot(a, b, preferred_element_type=f32)


def split(v):
    hi = v.astype(bf16)
    return hi, (v - hi.astype(f32)).astype(bf16)


def one_hot(size, t):
    hit = iota((size, t.shape[1]), 0, bf16) == t.astype(bf16)
    return jnp.where(hit, jnp.ones((), bf16), jnp.zeros((), bf16))


def block(i, size):
    if isinstance(i, int):
        return slice(i * size, (i + 1) * size)
    return pl.ds(pl.multiple_of(i * size, size), size)


def column_of(key, rank, first):
    off = rank - first
    fits = (off >= 0.0) & (off < 128.0)
    return jnp.where(fits, off + jnp.where(key >= 64, 128.0, 0.0), -1.0)


def head_row(k, half):
    return 2 * half + k if k < 2 else 4 + half


def body_row(k, half):
    return BODY * half + k


def place_all(rows_of, width, row_at, stride, key_ref, rank_ref, counts, out_ref, acc_ref, left_ref, col_ref, more=None):
    size = left_ref.shape[1]
    n = key_ref.shape[1] // size
    m = 64 * width
    ids = lax.broadcasted_iota(i32, (128, 128), 0).astype(f32)
    n_full = jnp.sum(jnp.where(counts > 128.0, 1.0, 0.0), axis=0, keepdims=True)
    hot = jnp.max(jnp.where(counts > 128.0, ids, -1.0), axis=0, keepdims=True)
    lone = jnp.concatenate([jnp.where(n_full <= 1.0, hot, -1.0)] * (size // 128), 1)

    def fill(rows, low, t):
        pick = one_hot(64, low)
        for k, r in enumerate(rows):
            hi, lo = split(r)
            left_ref[k * 64:(k + 1) * 64, :] = pick * hi
            left_ref[m + k * 64:m + (k + 1) * 64, :] = pick * lo
        col_ref[...] = one_hot(256, t)

    def flush(half, terms):
        for k in range(width):
            for o in range(2):
                at = pl.ds(o * 64 * stride + row_at(k, half), 64, stride=stride)
                lanes = slice(o * 128, (o + 1) * 128)
                out_ref[at, :] = sum(acc_ref[t, r + k * 64:r + (k + 1) * 64, lanes] for t, r in terms)

    for i in range(n):
        sl = block(i, size)
        key, rank = key_ref[0:1, sl], rank_ref[0:1, sl]
        rows = rows_of(sl)
        over = (key.astype(f32) == lone) & (rank >= 128.0)
        low = jnp.where(over, -1.0, (key & 63).astype(f32))
        fill(rows, low, jnp.where(over, rank - 128.0, column_of(key, rank, 0.0)))
        tail = jnp.concatenate([jnp.where(over, r, 0.0) for r in rows] + [jnp.zeros((8 - width, size), f32)], 0)
        hi = tail.astype(bf16).astype(f32)
        left_ref[2 * m:, :] = jnp.concatenate([hi, tail - hi], 0).astype(bf16)
        for k in range(2):
            lanes = slice(k * size // 2, (k + 1) * size // 2)
            acc_ref[2 * i + k] = nt(left_ref[:, lanes], col_ref[:, lanes])
    flush(0, [(k, part * m) for k in range(2 * n) for part in range(2)])
    spill = sum(acc_ref[k, 2 * m + 8 * j:2 * m + 8 * j + 8, :128] for k in range(2 * n) for j in range(2))
    base = jnp.max(jnp.maximum(hot, 0.0)).astype(i32) * stride
    for k in range(width):
        out_ref[pl.ds(base + row_at(k, 1), 1), :] = spill[k:k + 1]
    if more:
        more()

    @pl.when(jnp.max(n_full) > 1.0)
    def _():
        acc_ref[0] = jnp.zeros(acc_ref.shape[1:], f32)

        def again(i, carry):
            sl = block(i, size)
            key = key_ref[0:1, sl]
            fill(rows_of(sl), (key & 63).astype(f32), column_of(key, rank_ref[0:1, sl], 128.0))
            acc_ref[0, :2 * m, :] += nt(left_ref[:2 * m, :], col_ref[...])
            return carry

        lax.fori_loop(0, n, again, 0)
        flush(1, [(0, 0), (0, m)])


def around():
    x, y = lax.axis_index("gx"), lax.axis_index(WIDE)
    nx, ny = lax.axis_size("gx"), lax.axis_size(WIDE)

    def side(dx, dy):
        inside = (x + dx >= 0) & (x + dx < nx) & (y + dy >= 0) & (y + dy < ny)
        return inside, jnp.where(inside, (x + dx) * ny + y + dy, x * ny + y)

    return side


def head_kernel(far_ref, key_ref, a_ref, b_ref, v_ref, out_ref, rank_ref, count_ref, acc_ref, left_ref, col_ref, ut_ref, oh_ref, edge_ref, p_ref, sem):
    n = p_ref.shape[1] // RB
    copies = [pltpu.make_async_copy(far_ref, p_ref, sem.at[0]), pltpu.make_async_copy(v_ref, edge_ref, sem.at[1])]
    for copy in copies:
        copy.start()
    out_ref[...] = jnp.zeros(out_ref.shape, f32)
    before = lax.broadcasted_iota(i32, (256, 256), 0) < lax.broadcasted_iota(i32, (256, 256), 1)
    ut_ref[...] = jnp.where(before, 1.0, 0.0).astype(bf16)
    count_ref[...] = jnp.zeros(count_ref.shape, f32)

    def rank_block(i, carry):
        sl = block(i, RB)
        key = key_ref[0:1, sl].astype(f32)
        for k in range(RB // 256):
            oh_ref[k * 128:(k + 1) * 128, :] = one_hot(128, key[:, k * 256:(k + 1) * 256])
        res = nn(oh_ref[...], ut_ref[...])
        base = count_ref[...]
        ranks = []
        for k in range(RB // 256):
            hot = oh_ref[k * 128:(k + 1) * 128, :]
            low = base.astype(bf16)
            here = hot * (res[k * 128:(k + 1) * 128].astype(bf16) + jnp.concatenate([low, low], 1))
            tree = [here[j * 16:(j + 1) * 16] for j in range(8)]
            while len(tree) > 1:
                tree = [u + v for u, v in zip(tree[::2], tree[1::2])]
            ranks.append(jnp.sum(tree[0].astype(f32), axis=0, keepdims=True))
            pair = (hot[:, :128] + hot[:, 128:]).astype(f32)
            base = base + jnp.sum(pair, axis=1, keepdims=True)
        count_ref[...] = base
        rank_ref[0:1, sl] = jnp.concatenate(ranks, 1)
        return carry

    lax.fori_loop(0, n, rank_block, 0)
    for copy in copies:
        copy.wait()
    side = around()
    turned = [edge_ref[c].T for c in range(2)]

    def rows_of(sl):
        cell = (a_ref[0:1, sl] * 128 + b_ref[0:1, sl] + 1).astype(f32)
        return [p_ref[0:1, sl], p_ref[1:2, sl], cell]

    def halo():
        for dx in (-1, 0, 1):
            for dy in (-1, 0, 1):
                at = side(dx, dy)[1] * HEAD_ROWS + HALO
                for c in range(2):
                    if dx:
                        row = edge_ref.shape[1] - 1 if dx > 0 else 0
                        out_ref[pl.ds(at + c, 1), :] = edge_ref[c, row:row + 1, :]
                    elif dy:
                        col = edge_ref.shape[2] - 1 if dy > 0 else 0
                        for h in range(2):
                            out_ref[pl.ds(at + 2 * c + h, 1), :] = turned[c][col:col + 1, h * 128:(h + 1) * 128]

    place_all(rows_of, HEAD, head_row, HEAD_ROWS, key_ref, rank_ref, count_ref[...], out_ref, acc_ref, left_ref, col_ref, halo)


def body_kernel(p_ref, key_ref, rank_ref, count_ref, v_ref, out_ref, f_ref, acc_ref, left_ref, col_ref):
    out_ref[...] = jnp.zeros(out_ref.shape, f32)
    for c in range(2):
        hi, lo = split(v_ref[c].T)
        f_ref[c * 128:(c + 1) * 128, :] = hi
        f_ref[256 + c * 128:256 + (c + 1) * 128, :] = lo

    def rows_of(sl):
        return [p_ref[k:k + 1, sl] for k in range(2, 8)]

    place_all(rows_of, BODY, body_row, BODY_ROWS, key_ref, rank_ref, count_ref[...], out_ref, acc_ref, left_ref, col_ref)


def quad(t):
    return 0.5 * t * (t - 1.0), 1.0 - t * t, 0.5 * t * (t + 1.0)


def pick_of(hits, values, zero):
    out = zero
    for h, v in reversed(list(zip(hits, values))):
        out = jnp.where(h, v, out)
    return out


def interp_kernel(r_ref, f_ref, out_ref, cell_ref):
    S = 16
    side = around()

    def from_side(dx, dy, k):
        inside, who = side(dx, dy)
        row = r_ref[pl.ds(who * HEAD_ROWS + HALO + k, 1), :]
        return jnp.where(inside, row, 0.0)

    z4 = jnp.zeros((4, 128), f32)
    flat = jnp.concatenate([from_side(dx, 0, c) for c in range(2) for dx in (-1, 1)] + [z4], 0)
    west = jnp.concatenate([from_side(dx, -1, c) for c in range(2) for dx in (-1, 1)] + [z4], 0)
    east = jnp.concatenate([from_side(dx, 1, c) for c in range(2) for dx in (-1, 1)] + [z4], 0)
    west = jnp.broadcast_to(west[:, 127:128], (8, 128))
    east = jnp.broadcast_to(east[:, 0:1], (8, 128))
    tall = jnp.concatenate([from_side(0, dy, 2 * c + h) for h in range(2) for c in range(2) for dy in (-1, 1)], 0)
    sub = lax.broadcasted_iota(i32, (8, 128), 0)
    even = (sub & 1) == 0
    upper = sub < 4
    own = [(sub >> 1) == c for c in range(2)]
    own2 = [((sub >> 1) & 1) == c for c in range(2)]
    sub_f = sub.astype(f32)
    row_b = iota((16, 128), 0, bf16)
    zb = jnp.zeros((16, 128), bf16)
    z8 = jnp.zeros((8, 128), f32)

    def step(i, carry):
        groups = []
        for h in range(2):
            f, g, cell = [r_ref[pl.ds(i * (S * HEAD_ROWS) + head_row(k, h), S, stride=HEAD_ROWS), :] for k in range(3)]
            ci = cell.astype(i32) - 1
            cell_ref[pl.ds(i * (2 * S) + h, S, stride=2), :] = ci
            live = ci >= 0
            a = jnp.where(live, ci >> 7, 0)
            b = ci & 127
            half = jnp.where(live, 0.5, 0.0)
            wa = [half * w for w in quad(f)]
            wb = list(quad(g))
            hi = [w.astype(bf16).astype(f32) for w in wa]
            lo = [w - v for w, v in zip(wa, hi)]
            el, er = jnp.where(b == 0, wb[0], 0.0), jnp.where(b == 127, wb[2], 0.0)
            wb[0], wb[2] = wb[0] - el, wb[2] - er
            et, eb = jnp.where(a == 0, wa[0], 0.0), jnp.where(a == 255, wa[2], 0.0)
            at_a = [a - 1 + k for k in range(3)]
            w_half = [[jnp.where((t >> 7) == k, w, 0.0) for k in range(2)] for t, w in zip(at_a, wa)]
            groups.append(dict(
                w=hi + lo + [((a - 1) & 31).astype(f32), ((a - 1) >> 5).astype(f32)],
                wb=wb, start=((b - 1) & 7).astype(f32), q=((b - 1) >> 3) & 15, e=[el, er, et, eb],
                ia=[t & 127 for t in at_a], ib=[(b - 1 + k) & 127 for k in range(3)], w_half=w_half))

        def wide(x, j):
            return jnp.broadcast_to(x[j:j + 1], (8, 128))

        for u in range(S):
            spread = []
            for h in range(2):
                G = groups[h]
                packed = []
                for x in G["w"]:
                    y = wide(x, u)
                    packed.append(jnp.concatenate([y, y], 0).astype(bf16))
                his, los, start, q = packed[:3], packed[3:6], packed[6], packed[7]
                d = row_b - start
                near = [d == jnp.asarray(k, bf16) for k in range(3)]
                far = [d == jnp.asarray(k - 16, bf16) for k in range(3)]
                over = [d == jnp.asarray(k - 32, bf16) for k in (1, 2)]
                pieces = []
                for w in (his, los):
                    pieces.append((pick_of(near, w, zb), pick_of(far, w, zb), pick_of(over, w[1:], zb)))
                hit = q == jnp.asarray(-1, bf16)
                cols = [[], []]
                for j in range(8):
                    prev = hit
                    hit = q == jnp.asarray(j, bf16)
                    for k in range(2):
                        p0, p1, p2 = pieces[k]
                        cols[k].append(jnp.where(hit, p0, jnp.where(prev, p2, zb)))
                        cols[k].append(jnp.where(hit, p1, zb))
                spread.append([jnp.concatenate(c, 0) for c in cols])
            whi, wlo = [jnp.concatenate([spread[0][k], spread[1][k]], 1) for k in range(2)]
            two = nn(f_ref[...], whi)
            R = two[:256] + two[256:] + nn(f_ref[:256, :], wlo)
            for h in range(2):
                G = groups[h]
                V = R[:, 128 * h:128 * h + 128]
                d = sub_f - wide(G["start"], u)
                wb = [wide(w, u) for w in G["wb"]]
                c0 = pick_of([d == float(k) for k in range(3)], wb, z8)
                c1 = pick_of([d == float(k - 8) for k in (1, 2)], wb[1:], z8)
                q = wide(G["q"], u)
                bits = [(q & (1 << k)) != 0 for k in range(4)]

                def mux(v, b0, b1):
                    return jnp.where(b1, jnp.where(b0, v[3], v[2]), jnp.where(b0, v[1], v[0]))

                el, er, et, eb = [wide(e, u) for e in G["e"]]
                ga = [jnp.take_along_axis(tall, wide(t, u), axis=1) for t in G["ia"]]
                gb = [jnp.take_along_axis(flat, wide(t, u), axis=1) for t in G["ib"]]
                wh = [jnp.where(upper, wide(w[0], u), wide(w[1], u)) for w in G["w_half"]]
                beside = (wh[0] * ga[0] + wh[1] * ga[1] + wh[2] * ga[2]) * jnp.where(even, el, er)
                along = (wb[0] * gb[0] + wb[1] * gb[1] + wb[2] * gb[2] + el * west + er * east) * jnp.where(even, et, eb)
                for c in range(2):
                    r = [V[c * 128 + 8 * j:c * 128 + 8 * j + 8] for j in range(16)]
                    e = [mux([r[4 * m + t] for m in range(4)], bits[2], bits[3]) for t in range(4)]
                    e.append(mux([r[(4 * m + 4) % 16] for m in range(4)], bits[2], bits[3]))
                    first = mux(e[:4], bits[0], bits[1])
                    second = mux(e[1:], bits[0], bits[1])
                    total = first * c0 + second * c1 + jnp.where(own2[c], beside, 0.0) + jnp.where(own[c], along, 0.0)
                    row = PAD + 2 * (2 * u + h) + c
                    out_ref[pl.ds(i * (4 * S) + row, 1), :] = jnp.sum(total, axis=0, keepdims=True)
        return carry

    lax.fori_loop(0, OWNERS // S, step, 0)


def merge_kernel(d_ref, r1_ref, r2_ref, out_ref, tile_ref, sem):
    sub = lax.broadcasted_iota(i32, (8, 128), 0)
    top, mid = sub < 2, sub < 4
    copies = []
    for k in range(MERGES):
        for src in range(k * OWNERS // MERGES, (k + 1) * OWNERS // MERGES):
            for h in range(2):
                slot = 2 * src + h
                w = r1_ref[src * HEAD_ROWS + 2 * h:src * HEAD_ROWS + 2 * h + 8, :]
                at = src * BODY_ROWS + BODY * h - 2
                u = r2_ref[at:at + 8, :] if slot else pltpu.roll(r2_ref[0:8, :], 2, 0)
                d = d_ref[PAD + 2 * slot - 2:PAD + 2 * slot + 6, :]
                tile_ref[:, slot * 128:slot * 128 + 128] = jnp.where(top, w, jnp.where(mid, u + d, u))
        lanes = pl.ds(k * (tile_ref.shape[1] // MERGES), tile_ref.shape[1] // MERGES)
        copies.append(pltpu.make_async_copy(tile_ref.at[:, lanes], out_ref.at[:, lanes], sem.at[k]))
        copies[-1].start()
    for copy in copies:
        copy.wait()


def shape(*dims, dt=f32):
    return jax.ShapeDtypeStruct(dims, dt)


def held(*dims, dt=f32):
    return pltpu.VMEM(dims, dt)


def near_memory(x):
    return pltpu.with_memory_space_constraint(x, pltpu.VMEM)


def scratch(width, size):
    rows = 128 * width + 16
    return [pltpu.VMEM((16384 // size, rows, 256), f32), pltpu.VMEM((rows, size), bf16), pltpu.VMEM((256, size), bf16)]


def head(particles, key, a, b, velocity):
    n = particles.shape[1]
    return pl.pallas_call(
        head_kernel,
        out_shape=(held(OWNERS * HEAD_ROWS, 128), held(1, n), held(128, 128)),
        in_specs=[pl.BlockSpec(memory_space=pl.ANY)] + [VMEM] * 3 + [pl.BlockSpec(memory_space=pl.ANY)],
        out_specs=(VMEM,) * 3,
        scratch_shapes=scratch(HEAD, n // 2)
        + [pltpu.VMEM((256, 256), bf16), pltpu.VMEM((RB // 2, 256), bf16), pltpu.VMEM((2, 256, 128), f32), pltpu.VMEM((8, n), f32), pltpu.SemaphoreType.DMA((2,))],
        name="head",
    )(particles, key, a, b, velocity)


def body(particles, key, rank, count, velocity):
    return pl.pallas_call(
        body_kernel,
        out_shape=(held(OWNERS * BODY_ROWS, 128), held(512, 256, dt=bf16)),
        in_specs=[VMEM] * 5,
        out_specs=(VMEM,) * 2,
        scratch_shapes=scratch(BODY, particles.shape[1] // 2),
        name="body",
    )(particles, key, near_memory(rank), near_memory(count), velocity)


def interp(arrived, fields):
    return pl.pallas_call(
        interp_kernel,
        out_shape=(held(PAD + 4 * OWNERS + 8, 128), shape(2 * OWNERS, 128, dt=i32)),
        in_specs=[VMEM] * 2,
        out_specs=(VMEM,) * 2,
        name="interp",
    )(arrived, near_memory(fields))


def merge(moved, head_arrived, body_arrived):
    n = OWNERS * 256
    return pl.pallas_call(
        merge_kernel,
        out_shape=shape(8, n),
        in_specs=[VMEM] * 3,
        out_specs=pl.BlockSpec(memory_space=pl.ANY),
        scratch_shapes=[pltpu.VMEM((8, n), f32), pltpu.SemaphoreType.DMA((MERGES,))],
        name="merge",
    )(near_memory(moved), head_arrived, body_arrived)


def exchange(buckets, rows):
    out = lax.all_to_all(buckets.reshape(OWNERS, rows, 1, 128), ALL, 0, 0, tiled=True)
    return near_memory(out.reshape(OWNERS * rows, 128))


def shards(particles, dest_key, cell_a, cell_b, velocity):
    key, a, b = [v.reshape(1, -1) for v in (dest_key, cell_a, cell_b)]
    first, rank, count = head(particles, key, a, b, velocity)
    arrived = exchange(first, HEAD_ROWS)
    second, fields = body(particles, key, rank, count, velocity)
    rest = exchange(second, BODY_ROWS)
    moved, cell = interp(arrived, fields)
    return merge(moved, arrived, rest), cell.reshape(-1)


def solution(mesh):
    split_mesh = Mesh(mesh.devices.reshape(mesh.shape["gx"], 4, 4, mesh.shape["gz"]), ALL)
    in_specs = (P(None, ALL), P(ALL), P(ALL), P(ALL), P(None, "gx", WIDE))
    out_specs = (P(None, ALL), P(ALL))
    return jax.shard_map(shards, mesh=split_mesh, in_specs=in_specs, out_specs=out_specs, check_vma=False)
```

```python
import jax
import jax.numpy as jnp
from jax import lax
from jax.experimental import pallas as pl
from jax.experimental.pallas import tpu as pltpu
from jax.sharding import Mesh
from jax.sharding import PartitionSpec as P

f32, bf16, i32 = jnp.float32, jnp.bfloat16, jnp.int32
ALL = ("gx", "gy_0", "gy_1", "gz")
WIDE = ("gy_0", "gy_1", "gz")
OWNERS = 128
HEAD = 3
BODY = 6
HEAD_ROWS = 10
BODY_ROWS = 12
HALO = 6
PAD = 8
RB = 4096
MERGES = 4
VMEM = pl.BlockSpec(memory_space=pltpu.VMEM)


def iota(shape, dim, dt):
    return lax.broadcasted_iota(i32, shape, dim).astype(f32).astype(dt)


def nt(a, b):
    return lax.dot_general(a, b, (((1,), (1,)), ((), ())), preferred_element_type=f32)


def nn(a, b):
    return jnp.dot(a, b, preferred_element_type=f32)


def split(v):
    hi = v.astype(bf16)
    return hi, (v - hi.astype(f32)).astype(bf16)


def one_hot(size, t):
    hit = iota((size, t.shape[1]), 0, bf16) == t.astype(bf16)
    return jnp.where(hit, jnp.ones((), bf16), jnp.zeros((), bf16))


def block(i, size):
    if isinstance(i, int):
        return slice(i * size, (i + 1) * size)
    return pl.ds(pl.multiple_of(i * size, size), size)


def column_of(key, rank, first):
    off = rank - first
    fits = (off >= 0.0) & (off < 128.0)
    return jnp.where(fits, off + jnp.where(key >= 64, 128.0, 0.0), -1.0)


def head_row(k, half):
    return 2 * half + k if k < 2 else 4 + half


def body_row(k, half):
    return BODY * half + k


def place_all(rows_of, width, row_at, stride, key_ref, rank_ref, counts, out_ref, acc_ref, left_ref, col_ref, more=None):
    size = left_ref.shape[1]
    n = key_ref.shape[1] // size
    m = 64 * width
    ids = lax.broadcasted_iota(i32, (128, 128), 0).astype(f32)
    n_full = jnp.sum(jnp.where(counts > 128.0, 1.0, 0.0), axis=0, keepdims=True)
    hot = jnp.max(jnp.where(counts > 128.0, ids, -1.0), axis=0, keepdims=True)
    lone = jnp.concatenate([jnp.where(n_full <= 1.0, hot, -1.0)] * (size // 128), 1)

    def fill(rows, low, t):
        pick = one_hot(64, low)
        for k, r in enumerate(rows):
            hi, lo = split(r)
            left_ref[k * 64:(k + 1) * 64, :] = pick * hi
            left_ref[m + k * 64:m + (k + 1) * 64, :] = pick * lo
        col_ref[...] = one_hot(256, t)

    def flush(half, terms):
        for k in range(width):
            for o in range(2):
                at = pl.ds(o * 64 * stride + row_at(k, half), 64, stride=stride)
                lanes = slice(o * 128, (o + 1) * 128)
                out_ref[at, :] = sum(acc_ref[t, r + k * 64:r + (k + 1) * 64, lanes] for t, r in terms)

    for i in range(n):
        sl = block(i, size)
        key, rank = key_ref[0:1, sl], rank_ref[0:1, sl]
        rows = rows_of(sl)
        over = (key.astype(f32) == lone) & (rank >= 128.0)
        low = jnp.where(over, -1.0, (key & 63).astype(f32))
        fill(rows, low, jnp.where(over, rank - 128.0, column_of(key, rank, 0.0)))
        tail = jnp.concatenate([jnp.where(over, r, 0.0) for r in rows] + [jnp.zeros((8 - width, size), f32)], 0)
        hi = tail.astype(bf16).astype(f32)
        left_ref[2 * m:, :] = jnp.concatenate([hi, tail - hi], 0).astype(bf16)
        for k in range(2):
            lanes = slice(k * size // 2, (k + 1) * size // 2)
            acc_ref[2 * i + k] = nt(left_ref[:, lanes], col_ref[:, lanes])
    flush(0, [(k, part * m) for k in range(2 * n) for part in range(2)])
    spill = sum(acc_ref[k, 2 * m + 8 * j:2 * m + 8 * j + 8, :128] for k in range(2 * n) for j in range(2))
    base = jnp.max(jnp.maximum(hot, 0.0)).astype(i32) * stride
    for k in range(width):
        out_ref[pl.ds(base + row_at(k, 1), 1), :] = spill[k:k + 1]
    if more:
        more()

    @pl.when(jnp.max(n_full) > 1.0)
    def _():
        acc_ref[0] = jnp.zeros(acc_ref.shape[1:], f32)

        def again(i, carry):
            sl = block(i, size)
            key = key_ref[0:1, sl]
            fill(rows_of(sl), (key & 63).astype(f32), column_of(key, rank_ref[0:1, sl], 128.0))
            acc_ref[0, :2 * m, :] += nt(left_ref[:2 * m, :], col_ref[...])
            return carry

        lax.fori_loop(0, n, again, 0)
        flush(1, [(0, 0), (0, m)])


def around():
    x, y = lax.axis_index("gx"), lax.axis_index(WIDE)
    nx, ny = lax.axis_size("gx"), lax.axis_size(WIDE)

    def side(dx, dy):
        inside = (x + dx >= 0) & (x + dx < nx) & (y + dy >= 0) & (y + dy < ny)
        return inside, jnp.where(inside, (x + dx) * ny + y + dy, x * ny + y)

    return side


def head_kernel(far_ref, far_key_ref, far_a_ref, far_b_ref, v_ref, out_ref, rank_ref, count_ref, acc_ref, left_ref, col_ref, ut_ref, oh_ref, edge_ref, p_ref, key_ref, a_ref, b_ref, sem):
    n = p_ref.shape[1] // RB
    pairs = ((far_key_ref, key_ref), (far_a_ref, a_ref), (far_b_ref, b_ref), (far_ref, p_ref), (v_ref, edge_ref))
    copies = [pltpu.make_async_copy(source, target, sem.at[k]) for k, (source, target) in enumerate(pairs)]
    for copy in copies:
        copy.start()
    out_ref[...] = jnp.zeros(out_ref.shape, f32)
    before = lax.broadcasted_iota(i32, (256, 256), 0) < lax.broadcasted_iota(i32, (256, 256), 1)
    ut_ref[...] = jnp.where(before, 1.0, 0.0).astype(bf16)
    count_ref[...] = jnp.zeros(count_ref.shape, f32)

    def rank_block(i, carry):
        sl = block(i, RB)
        key = key_ref[0:1, sl].astype(f32)
        for k in range(RB // 256):
            oh_ref[k * 128:(k + 1) * 128, :] = one_hot(128, key[:, k * 256:(k + 1) * 256])
        res = nn(oh_ref[...], ut_ref[...])
        base = count_ref[...]
        ranks = []
        for k in range(RB // 256):
            hot = oh_ref[k * 128:(k + 1) * 128, :]
            low = base.astype(bf16)
            here = hot * (res[k * 128:(k + 1) * 128].astype(bf16) + jnp.concatenate([low, low], 1))
            tree = [here[j * 16:(j + 1) * 16] for j in range(8)]
            while len(tree) > 1:
                tree = [u + v for u, v in zip(tree[::2], tree[1::2])]
            ranks.append(jnp.sum(tree[0].astype(f32), axis=0, keepdims=True))
            pair = (hot[:, :128] + hot[:, 128:]).astype(f32)
            base = base + jnp.sum(pair, axis=1, keepdims=True)
        count_ref[...] = base
        rank_ref[0:1, sl] = jnp.concatenate(ranks, 1)
        return carry

    copies[0].wait()
    lax.fori_loop(0, n, rank_block, 0)
    for copy in copies[1:]:
        copy.wait()
    side = around()
    turned = [edge_ref[c].T for c in range(2)]

    def rows_of(sl):
        cell = (a_ref[0:1, sl] * 128 + b_ref[0:1, sl] + 1).astype(f32)
        return [p_ref[0:1, sl], p_ref[1:2, sl], cell]

    def halo():
        for dx in (-1, 0, 1):
            for dy in (-1, 0, 1):
                at = side(dx, dy)[1] * HEAD_ROWS + HALO
                for c in range(2):
                    if dx:
                        row = edge_ref.shape[1] - 1 if dx > 0 else 0
                        out_ref[pl.ds(at + c, 1), :] = edge_ref[c, row:row + 1, :]
                    elif dy:
                        col = edge_ref.shape[2] - 1 if dy > 0 else 0
                        for h in range(2):
                            out_ref[pl.ds(at + 2 * c + h, 1), :] = turned[c][col:col + 1, h * 128:(h + 1) * 128]

    place_all(rows_of, HEAD, head_row, HEAD_ROWS, key_ref, rank_ref, count_ref[...], out_ref, acc_ref, left_ref, col_ref, halo)


def body_kernel(p_ref, key_ref, rank_ref, count_ref, v_ref, out_ref, f_ref, acc_ref, left_ref, col_ref):
    out_ref[...] = jnp.zeros(out_ref.shape, f32)
    for c in range(2):
        hi, lo = split(v_ref[c].T)
        f_ref[c * 128:(c + 1) * 128, :] = hi
        f_ref[256 + c * 128:256 + (c + 1) * 128, :] = lo

    def rows_of(sl):
        return [p_ref[k:k + 1, sl] for k in range(2, 8)]

    place_all(rows_of, BODY, body_row, BODY_ROWS, key_ref, rank_ref, count_ref[...], out_ref, acc_ref, left_ref, col_ref)


def quad(t):
    return 0.5 * t * (t - 1.0), 1.0 - t * t, 0.5 * t * (t + 1.0)


def pick_of(hits, values, zero):
    out = zero
    for h, v in reversed(list(zip(hits, values))):
        out = jnp.where(h, v, out)
    return out


def interp_kernel(r_ref, f_ref, out_ref, cell_ref):
    S = 16
    side = around()

    def from_side(dx, dy, k):
        inside, who = side(dx, dy)
        row = r_ref[pl.ds(who * HEAD_ROWS + HALO + k, 1), :]
        return jnp.where(inside, row, 0.0)

    z4 = jnp.zeros((4, 128), f32)
    flat = jnp.concatenate([from_side(dx, 0, c) for c in range(2) for dx in (-1, 1)] + [z4], 0)
    west = jnp.concatenate([from_side(dx, -1, c) for c in range(2) for dx in (-1, 1)] + [z4], 0)
    east = jnp.concatenate([from_side(dx, 1, c) for c in range(2) for dx in (-1, 1)] + [z4], 0)
    west = jnp.broadcast_to(west[:, 127:128], (8, 128))
    east = jnp.broadcast_to(east[:, 0:1], (8, 128))
    tall = jnp.concatenate([from_side(0, dy, 2 * c + h) for h in range(2) for c in range(2) for dy in (-1, 1)], 0)
    sub = lax.broadcasted_iota(i32, (8, 128), 0)
    even = (sub & 1) == 0
    upper = sub < 4
    own = [(sub >> 1) == c for c in range(2)]
    own2 = [((sub >> 1) & 1) == c for c in range(2)]
    sub_f = sub.astype(f32)
    row_b = iota((16, 128), 0, bf16)
    zb = jnp.zeros((16, 128), bf16)
    z8 = jnp.zeros((8, 128), f32)

    def step(i, carry):
        groups = []
        for h in range(2):
            f, g, cell = [r_ref[pl.ds(i * (S * HEAD_ROWS) + head_row(k, h), S, stride=HEAD_ROWS), :] for k in range(3)]
            ci = cell.astype(i32) - 1
            cell_ref[pl.ds(i * (2 * S) + h, S, stride=2), :] = ci
            live = ci >= 0
            a = jnp.where(live, ci >> 7, 0)
            b = ci & 127
            half = jnp.where(live, 0.5, 0.0)
            wa = [half * w for w in quad(f)]
            wb = list(quad(g))
            hi = [w.astype(bf16).astype(f32) for w in wa]
            lo = [w - v for w, v in zip(wa, hi)]
            el, er = jnp.where(b == 0, wb[0], 0.0), jnp.where(b == 127, wb[2], 0.0)
            wb[0], wb[2] = wb[0] - el, wb[2] - er
            et, eb = jnp.where(a == 0, wa[0], 0.0), jnp.where(a == 255, wa[2], 0.0)
            at_a = [a - 1 + k for k in range(3)]
            w_half = [[jnp.where((t >> 7) == k, w, 0.0) for k in range(2)] for t, w in zip(at_a, wa)]
            groups.append(dict(
                w=hi + lo + [((a - 1) & 31).astype(f32), ((a - 1) >> 5).astype(f32)],
                wb=wb, start=((b - 1) & 7).astype(f32), q=((b - 1) >> 3) & 15, e=[el, er, et, eb],
                ia=[t & 127 for t in at_a], ib=[(b - 1 + k) & 127 for k in range(3)], w_half=w_half))

        def wide(x, j):
            return jnp.broadcast_to(x[j:j + 1], (8, 128))

        for u in range(S):
            spread = []
            for h in range(2):
                G = groups[h]
                packed = []
                for x in G["w"]:
                    y = wide(x, u)
                    packed.append(jnp.concatenate([y, y], 0).astype(bf16))
                his, los, start, q = packed[:3], packed[3:6], packed[6], packed[7]
                d = row_b - start
                near = [d == jnp.asarray(k, bf16) for k in range(3)]
                far = [d == jnp.asarray(k - 16, bf16) for k in range(3)]
                over = [d == jnp.asarray(k - 32, bf16) for k in (1, 2)]
                pieces = []
                for w in (his, los):
                    pieces.append((pick_of(near, w, zb), pick_of(far, w, zb), pick_of(over, w[1:], zb)))
                hit = q == jnp.asarray(-1, bf16)
                cols = [[], []]
                for j in range(8):
                    prev = hit
                    hit = q == jnp.asarray(j, bf16)
                    for k in range(2):
                        p0, p1, p2 = pieces[k]
                        cols[k].append(jnp.where(hit, p0, jnp.where(prev, p2, zb)))
                        cols[k].append(jnp.where(hit, p1, zb))
                spread.append([jnp.concatenate(c, 0) for c in cols])
            whi, wlo = [jnp.concatenate([spread[0][k], spread[1][k]], 1) for k in range(2)]
            two = nn(f_ref[...], whi)
            R = two[:256] + two[256:] + nn(f_ref[:256, :], wlo)
            for h in range(2):
                G = groups[h]
                V = R[:, 128 * h:128 * h + 128]
                d = sub_f - wide(G["start"], u)
                wb = [wide(w, u) for w in G["wb"]]
                c0 = pick_of([d == float(k) for k in range(3)], wb, z8)
                c1 = pick_of([d == float(k - 8) for k in (1, 2)], wb[1:], z8)
                q = wide(G["q"], u)
                bits = [(q & (1 << k)) != 0 for k in range(4)]

                def mux(v, b0, b1):
                    return jnp.where(b1, jnp.where(b0, v[3], v[2]), jnp.where(b0, v[1], v[0]))

                el, er, et, eb = [wide(e, u) for e in G["e"]]
                ga = [jnp.take_along_axis(tall, wide(t, u), axis=1) for t in G["ia"]]
                gb = [jnp.take_along_axis(flat, wide(t, u), axis=1) for t in G["ib"]]
                wh = [jnp.where(upper, wide(w[0], u), wide(w[1], u)) for w in G["w_half"]]
                beside = (wh[0] * ga[0] + wh[1] * ga[1] + wh[2] * ga[2]) * jnp.where(even, el, er)
                along = (wb[0] * gb[0] + wb[1] * gb[1] + wb[2] * gb[2] + el * west + er * east) * jnp.where(even, et, eb)
                for c in range(2):
                    r = [V[c * 128 + 8 * j:c * 128 + 8 * j + 8] for j in range(16)]
                    e = [mux([r[4 * m + t] for m in range(4)], bits[2], bits[3]) for t in range(4)]
                    e.append(mux([r[(4 * m + 4) % 16] for m in range(4)], bits[2], bits[3]))
                    first = mux(e[:4], bits[0], bits[1])
                    second = mux(e[1:], bits[0], bits[1])
                    total = first * c0 + second * c1 + jnp.where(own2[c], beside, 0.0) + jnp.where(own[c], along, 0.0)
                    row = PAD + 2 * (2 * u + h) + c
                    out_ref[pl.ds(i * (4 * S) + row, 1), :] = jnp.sum(total, axis=0, keepdims=True)
        return carry

    lax.fori_loop(0, OWNERS // S, step, 0)


def merge_kernel(d_ref, r1_ref, r2_ref, out_ref, tile_ref, sem):
    sub = lax.broadcasted_iota(i32, (8, 128), 0)
    top, mid = sub < 2, sub < 4
    copies = []
    for k in range(MERGES):
        for src in range(k * OWNERS // MERGES, (k + 1) * OWNERS // MERGES):
            for h in range(2):
                slot = 2 * src + h
                w = r1_ref[src * HEAD_ROWS + 2 * h:src * HEAD_ROWS + 2 * h + 8, :]
                at = src * BODY_ROWS + BODY * h - 2
                u = r2_ref[at:at + 8, :] if slot else pltpu.roll(r2_ref[0:8, :], 2, 0)
                d = d_ref[PAD + 2 * slot - 2:PAD + 2 * slot + 6, :]
                tile_ref[:, slot * 128:slot * 128 + 128] = jnp.where(top, w, jnp.where(mid, u + d, u))
        lanes = pl.ds(k * (tile_ref.shape[1] // MERGES), tile_ref.shape[1] // MERGES)
        copies.append(pltpu.make_async_copy(tile_ref.at[:, lanes], out_ref.at[:, lanes], sem.at[k]))
        copies[-1].start()
    for copy in copies:
        copy.wait()


def shape(*dims, dt=f32):
    return jax.ShapeDtypeStruct(dims, dt)


def held(*dims, dt=f32):
    return pltpu.VMEM(dims, dt)


def near_memory(x):
    return pltpu.with_memory_space_constraint(x, pltpu.VMEM)


def scratch(width, size):
    rows = 128 * width + 16
    return [pltpu.VMEM((16384 // size, rows, 256), f32), pltpu.VMEM((rows, size), bf16), pltpu.VMEM((256, size), bf16)]


def head(particles, key, a, b, velocity):
    n = particles.shape[1]
    return pl.pallas_call(
        head_kernel,
        out_shape=(held(OWNERS * HEAD_ROWS, 128), held(1, n), held(128, 128)),
        in_specs=[pl.BlockSpec(memory_space=pl.ANY)] * 5,
        out_specs=(VMEM,) * 3,
        scratch_shapes=scratch(HEAD, n // 2)
        + [pltpu.VMEM((256, 256), bf16), pltpu.VMEM((RB // 2, 256), bf16), pltpu.VMEM((2, 256, 128), f32), pltpu.VMEM((8, n), f32)]
        + [pltpu.VMEM((1, n), i32)] * 3 + [pltpu.SemaphoreType.DMA((5,))],
        name="head",
    )(particles, key, a, b, velocity)


def body(particles, key, rank, count, velocity):
    return pl.pallas_call(
        body_kernel,
        out_shape=(held(OWNERS * BODY_ROWS, 128), held(512, 256, dt=bf16)),
        in_specs=[VMEM] * 5,
        out_specs=(VMEM,) * 2,
        scratch_shapes=scratch(BODY, particles.shape[1] // 2),
        name="body",
    )(particles, key, near_memory(rank), near_memory(count), velocity)


def interp(arrived, fields):
    return pl.pallas_call(
        interp_kernel,
        out_shape=(held(PAD + 4 * OWNERS + 8, 128), shape(2 * OWNERS, 128, dt=i32)),
        in_specs=[VMEM] * 2,
        out_specs=(VMEM,) * 2,
        name="interp",
    )(arrived, near_memory(fields))


def merge(moved, head_arrived, body_arrived):
    n = OWNERS * 256
    return pl.pallas_call(
        merge_kernel,
        out_shape=shape(8, n),
        in_specs=[VMEM] * 3,
        out_specs=pl.BlockSpec(memory_space=pl.ANY),
        scratch_shapes=[pltpu.VMEM((8, n), f32), pltpu.SemaphoreType.DMA((MERGES,))],
        name="merge",
    )(near_memory(moved), head_arrived, body_arrived)


def exchange(buckets, rows):
    out = lax.all_to_all(buckets.reshape(OWNERS, rows, 1, 128), ALL, 0, 0, tiled=True)
    return near_memory(out.reshape(OWNERS * rows, 128))


def shards(particles, dest_key, cell_a, cell_b, velocity):
    key, a, b = [v.reshape(1, -1) for v in (dest_key, cell_a, cell_b)]
    first, rank, count = head(particles, key, a, b, velocity)
    arrived = exchange(first, HEAD_ROWS)
    second, fields = body(particles, key, rank, count, velocity)
    rest = exchange(second, BODY_ROWS)
    moved, cell = interp(arrived, fields)
    return merge(moved, arrived, rest), cell.reshape(-1)


def solution(mesh):
    split_mesh = Mesh(mesh.devices.reshape(mesh.shape["gx"], 4, 4, mesh.shape["gz"]), ALL)
    in_specs = (P(None, ALL), P(ALL), P(ALL), P(ALL), P(None, "gx", WIDE))
    out_specs = (P(None, ALL), P(ALL))
    return jax.shard_map(shards, mesh=split_mesh, in_specs=in_specs, out_specs=out_specs, check_vma=False)
```

```python
import jax
import jax.numpy as jnp
from jax import lax
from jax.experimental import pallas as pl
from jax.experimental.pallas import tpu as pltpu
from jax.sharding import Mesh
from jax.sharding import PartitionSpec as P

f32, bf16, i32 = jnp.float32, jnp.bfloat16, jnp.int32
ALL = ("gx", "gy_0", "gy_1", "gz")
WIDE = ("gy_0", "gy_1", "gz")
OWNERS = 128
HEAD = 3
BODY = 6
HEAD_ROWS = 10
BODY_ROWS = 12
HALO = 6
PAD = 8
RB = 4096
MERGES = 4
VMEM = pl.BlockSpec(memory_space=pltpu.VMEM)


def iota(shape, dim, dt):
    return lax.broadcasted_iota(i32, shape, dim).astype(f32).astype(dt)


def nt(a, b):
    return lax.dot_general(a, b, (((1,), (1,)), ((), ())), preferred_element_type=f32)


def nn(a, b):
    return jnp.dot(a, b, preferred_element_type=f32)


def split(v):
    hi = v.astype(bf16)
    return hi, (v - hi.astype(f32)).astype(bf16)


def one_hot(size, t):
    hit = iota((size, t.shape[1]), 0, bf16) == t.astype(bf16)
    return jnp.where(hit, jnp.ones((), bf16), jnp.zeros((), bf16))


def block(i, size):
    if isinstance(i, int):
        return slice(i * size, (i + 1) * size)
    return pl.ds(pl.multiple_of(i * size, size), size)


def column_of(key, rank, first):
    off = rank - first
    fits = (off >= 0.0) & (off < 128.0)
    return jnp.where(fits, off + jnp.where(key >= 64, 128.0, 0.0), -1.0)


def head_row(k, half):
    return 2 * half + k if k < 2 else 4 + half


def body_row(k, half):
    return BODY * half + k


def place_all(rows_of, width, row_at, stride, key_ref, rank_ref, counts, out_ref, acc_ref, left_ref, col_ref, more=None):
    size = left_ref.shape[1]
    n = key_ref.shape[1] // size
    m = 64 * width
    ids = lax.broadcasted_iota(i32, (128, 128), 0).astype(f32)
    n_full = jnp.sum(jnp.where(counts > 128.0, 1.0, 0.0), axis=0, keepdims=True)
    hot = jnp.max(jnp.where(counts > 128.0, ids, -1.0), axis=0, keepdims=True)
    lone = jnp.concatenate([jnp.where(n_full <= 1.0, hot, -1.0)] * (size // 128), 1)

    def fill(rows, low, t):
        pick = one_hot(64, low)
        for k, r in enumerate(rows):
            hi, lo = split(r)
            left_ref[k * 64:(k + 1) * 64, :] = pick * hi
            left_ref[m + k * 64:m + (k + 1) * 64, :] = pick * lo
        col_ref[...] = one_hot(256, t)

    def flush(half, terms):
        for k in range(width):
            for o in range(2):
                at = pl.ds(o * 64 * stride + row_at(k, half), 64, stride=stride)
                lanes = slice(o * 128, (o + 1) * 128)
                out_ref[at, :] = sum(acc_ref[t, r + k * 64:r + (k + 1) * 64, lanes] for t, r in terms)

    for i in range(n):
        sl = block(i, size)
        key, rank = key_ref[0:1, sl], rank_ref[0:1, sl]
        rows = rows_of(sl)
        over = (key.astype(f32) == lone) & (rank >= 128.0)
        low = jnp.where(over, -1.0, (key & 63).astype(f32))
        fill(rows, low, jnp.where(over, rank - 128.0, column_of(key, rank, 0.0)))
        tail = jnp.concatenate([jnp.where(over, r, 0.0) for r in rows] + [jnp.zeros((8 - width, size), f32)], 0)
        hi = tail.astype(bf16).astype(f32)
        left_ref[2 * m:, :] = jnp.concatenate([hi, tail - hi], 0).astype(bf16)
        for k in range(2):
            lanes = slice(k * size // 2, (k + 1) * size // 2)
            acc_ref[2 * i + k] = nt(left_ref[:, lanes], col_ref[:, lanes])
    flush(0, [(k, part * m) for k in range(2 * n) for part in range(2)])
    spill = sum(acc_ref[k, 2 * m + 8 * j:2 * m + 8 * j + 8, :128] for k in range(2 * n) for j in range(2))
    base = jnp.max(jnp.maximum(hot, 0.0)).astype(i32) * stride
    for k in range(width):
        out_ref[pl.ds(base + row_at(k, 1), 1), :] = spill[k:k + 1]
    if more:
        more()

    @pl.when(jnp.max(n_full) > 1.0)
    def _():
        acc_ref[0] = jnp.zeros(acc_ref.shape[1:], f32)

        def again(i, carry):
            sl = block(i, size)
            key = key_ref[0:1, sl]
            fill(rows_of(sl), (key & 63).astype(f32), column_of(key, rank_ref[0:1, sl], 128.0))
            acc_ref[0, :2 * m, :] += nt(left_ref[:2 * m, :], col_ref[...])
            return carry

        lax.fori_loop(0, n, again, 0)
        flush(1, [(0, 0), (0, m)])


def around():
    x, y = lax.axis_index("gx"), lax.axis_index(WIDE)
    nx, ny = lax.axis_size("gx"), lax.axis_size(WIDE)

    def side(dx, dy):
        inside = (x + dx >= 0) & (x + dx < nx) & (y + dy >= 0) & (y + dy < ny)
        return inside, jnp.where(inside, (x + dx) * ny + y + dy, x * ny + y)

    return side


def head_kernel(far_ref, key_ref, a_ref, b_ref, v_ref, out_ref, rank_ref, count_ref, acc_ref, left_ref, col_ref, ut_ref, oh_ref, edge_ref, p_ref, sem):
    n = p_ref.shape[1] // RB
    copies = [pltpu.make_async_copy(far_ref, p_ref, sem.at[0]), pltpu.make_async_copy(v_ref, edge_ref, sem.at[1])]
    for copy in copies:
        copy.start()
    out_ref[...] = jnp.zeros(out_ref.shape, f32)
    before = lax.broadcasted_iota(i32, (256, 256), 0) < lax.broadcasted_iota(i32, (256, 256), 1)
    ut_ref[...] = jnp.where(before, 1.0, 0.0).astype(bf16)
    count_ref[...] = jnp.zeros(count_ref.shape, f32)

    def rank_block(i, carry):
        sl = block(i, RB)
        key = key_ref[0:1, sl].astype(f32)
        for k in range(RB // 256):
            oh_ref[k * 128:(k + 1) * 128, :] = one_hot(128, key[:, k * 256:(k + 1) * 256])
        res = nn(oh_ref[...], ut_ref[...])
        base = count_ref[...]
        ranks = []
        for k in range(RB // 256):
            hot = oh_ref[k * 128:(k + 1) * 128, :]
            low = base.astype(bf16)
            here = hot * (res[k * 128:(k + 1) * 128].astype(bf16) + jnp.concatenate([low, low], 1))
            tree = [here[j * 16:(j + 1) * 16] for j in range(8)]
            while len(tree) > 1:
                tree = [u + v for u, v in zip(tree[::2], tree[1::2])]
            ranks.append(jnp.sum(tree[0].astype(f32), axis=0, keepdims=True))
            pair = (hot[:, :128] + hot[:, 128:]).astype(f32)
            base = base + jnp.sum(pair, axis=1, keepdims=True)
        count_ref[...] = base
        rank_ref[0:1, sl] = jnp.concatenate(ranks, 1)
        return carry

    lax.fori_loop(0, n, rank_block, 0)
    for copy in copies:
        copy.wait()
    side = around()
    turned = [edge_ref[c].T for c in range(2)]

    def rows_of(sl):
        cell = (a_ref[0:1, sl] * 128 + b_ref[0:1, sl] + 1).astype(f32)
        return [p_ref[0:1, sl], p_ref[1:2, sl], cell]

    def halo():
        for dx in (-1, 0, 1):
            for dy in (-1, 0, 1):
                at = side(dx, dy)[1] * HEAD_ROWS + HALO
                for c in range(2):
                    if dx:
                        row = edge_ref.shape[1] - 1 if dx > 0 else 0
                        out_ref[pl.ds(at + c, 1), :] = edge_ref[c, row:row + 1, :]
                    elif dy:
                        col = edge_ref.shape[2] - 1 if dy > 0 else 0
                        for h in range(2):
                            out_ref[pl.ds(at + 2 * c + h, 1), :] = turned[c][col:col + 1, h * 128:(h + 1) * 128]

    place_all(rows_of, HEAD, head_row, HEAD_ROWS, key_ref, rank_ref, count_ref[...], out_ref, acc_ref, left_ref, col_ref, halo)


def body_kernel(p_ref, key_ref, rank_ref, count_ref, v_ref, out_ref, f_ref, acc_ref, left_ref, col_ref):
    out_ref[...] = jnp.zeros(out_ref.shape, f32)
    for c in range(2):
        hi, lo = split(v_ref[c].T)
        f_ref[c * 128:(c + 1) * 128, :] = hi
        f_ref[256 + c * 128:256 + (c + 1) * 128, :] = lo

    def rows_of(sl):
        return [p_ref[k:k + 1, sl] for k in range(2, 8)]

    place_all(rows_of, BODY, body_row, BODY_ROWS, key_ref, rank_ref, count_ref[...], out_ref, acc_ref, left_ref, col_ref)


def quad(t):
    return 0.5 * t * (t - 1.0), 1.0 - t * t, 0.5 * t * (t + 1.0)


def pick_of(hits, values, zero):
    out = zero
    for h, v in reversed(list(zip(hits, values))):
        out = jnp.where(h, v, out)
    return out


def interp_kernel(r_ref, f_ref, out_ref, cell_ref):
    S = 16
    side = around()

    def from_side(dx, dy, k):
        inside, who = side(dx, dy)
        row = r_ref[pl.ds(who * HEAD_ROWS + HALO + k, 1), :]
        return jnp.where(inside, row, 0.0)

    z4 = jnp.zeros((4, 128), f32)
    flat = jnp.concatenate([from_side(dx, 0, c) for c in range(2) for dx in (-1, 1)] + [z4], 0)
    west = jnp.concatenate([from_side(dx, -1, c) for c in range(2) for dx in (-1, 1)] + [z4], 0)
    east = jnp.concatenate([from_side(dx, 1, c) for c in range(2) for dx in (-1, 1)] + [z4], 0)
    west = jnp.broadcast_to(west[:, 127:128], (8, 128))
    east = jnp.broadcast_to(east[:, 0:1], (8, 128))
    tall = jnp.concatenate([from_side(0, dy, 2 * c + h) for h in range(2) for c in range(2) for dy in (-1, 1)], 0)
    sub = lax.broadcasted_iota(i32, (8, 128), 0)
    even = (sub & 1) == 0
    upper = sub < 4
    own = [(sub >> 1) == c for c in range(2)]
    own2 = [((sub >> 1) & 1) == c for c in range(2)]
    sub_f = sub.astype(f32)
    row_b = iota((16, 128), 0, bf16)
    zb = jnp.zeros((16, 128), bf16)
    z8 = jnp.zeros((8, 128), f32)

    def step(i, carry):
        groups = []
        for h in range(2):
            f, g, cell = [r_ref[pl.ds(i * (S * HEAD_ROWS) + head_row(k, h), S, stride=HEAD_ROWS), :] for k in range(3)]
            ci = cell.astype(i32) - 1
            cell_ref[pl.ds(i * (2 * S) + h, S, stride=2), :] = ci
            live = ci >= 0
            a = jnp.where(live, ci >> 7, 0)
            b = ci & 127
            half = jnp.where(live, 0.5, 0.0)
            wa = [half * w for w in quad(f)]
            wb = list(quad(g))
            hi = [w.astype(bf16).astype(f32) for w in wa]
            lo = [w - v for w, v in zip(wa, hi)]
            el, er = jnp.where(b == 0, wb[0], 0.0), jnp.where(b == 127, wb[2], 0.0)
            wb[0], wb[2] = wb[0] - el, wb[2] - er
            et, eb = jnp.where(a == 0, wa[0], 0.0), jnp.where(a == 255, wa[2], 0.0)
            at_a = [a - 1 + k for k in range(3)]
            w_half = [[jnp.where((t >> 7) == k, w, 0.0) for k in range(2)] for t, w in zip(at_a, wa)]
            groups.append(dict(
                w=hi + lo + [((a - 1) & 31).astype(f32), ((a - 1) >> 5).astype(f32)],
                wb=wb, start=((b - 1) & 7).astype(f32), q=((b - 1) >> 3) & 15, e=[el, er, et, eb],
                ia=[t & 127 for t in at_a], ib=[(b - 1 + k) & 127 for k in range(3)], w_half=w_half))

        def wide(x, j):
            return jnp.broadcast_to(x[j:j + 1], (8, 128))

        for u in range(S):
            spread = []
            for h in range(2):
                G = groups[h]
                packed = []
                for x in G["w"]:
                    y = wide(x, u)
                    packed.append(jnp.concatenate([y, y], 0).astype(bf16))
                his, los, start, q = packed[:3], packed[3:6], packed[6], packed[7]
                d = row_b - start
                near = [d == jnp.asarray(k, bf16) for k in range(3)]
                far = [d == jnp.asarray(k - 16, bf16) for k in range(3)]
                over = [d == jnp.asarray(k - 32, bf16) for k in (1, 2)]
                pieces = []
                for w in (his, los):
                    pieces.append((pick_of(near, w, zb), pick_of(far, w, zb), pick_of(over, w[1:], zb)))
                hit = q == jnp.asarray(-1, bf16)
                cols = [[], []]
                for j in range(8):
                    prev = hit
                    hit = q == jnp.asarray(j, bf16)
                    for k in range(2):
                        p0, p1, p2 = pieces[k]
                        cols[k].append(jnp.where(hit, p0, jnp.where(prev, p2, zb)))
                        cols[k].append(jnp.where(hit, p1, zb))
                spread.append([jnp.concatenate(c, 0) for c in cols])
            whi, wlo = [jnp.concatenate([spread[0][k], spread[1][k]], 1) for k in range(2)]
            two = nn(f_ref[...], whi)
            R = two[:256] + two[256:] + nn(f_ref[:256, :], wlo)
            for h in range(2):
                G = groups[h]
                V = R[:, 128 * h:128 * h + 128]
                d = sub_f - wide(G["start"], u)
                wb = [wide(w, u) for w in G["wb"]]
                c0 = pick_of([d == float(k) for k in range(3)], wb, z8)
                c1 = pick_of([d == float(k - 8) for k in (1, 2)], wb[1:], z8)
                q = wide(G["q"], u)
                bits = [(q & (1 << k)) != 0 for k in range(4)]

                def mux(v, b0, b1):
                    return jnp.where(b1, jnp.where(b0, v[3], v[2]), jnp.where(b0, v[1], v[0]))

                el, er, et, eb = [wide(e, u) for e in G["e"]]
                ga = [jnp.take_along_axis(tall, wide(t, u), axis=1) for t in G["ia"]]
                gb = [jnp.take_along_axis(flat, wide(t, u), axis=1) for t in G["ib"]]
                wh = [jnp.where(upper, wide(w[0], u), wide(w[1], u)) for w in G["w_half"]]
                beside = (wh[0] * ga[0] + wh[1] * ga[1] + wh[2] * ga[2]) * jnp.where(even, el, er)
                along = (wb[0] * gb[0] + wb[1] * gb[1] + wb[2] * gb[2] + el * west + er * east) * jnp.where(even, et, eb)
                for c in range(2):
                    r = [V[c * 128 + 8 * j:c * 128 + 8 * j + 8] for j in range(16)]
                    e = [mux([r[4 * m + t] for m in range(4)], bits[2], bits[3]) for t in range(4)]
                    e.append(mux([r[(4 * m + 4) % 16] for m in range(4)], bits[2], bits[3]))
                    first = mux(e[:4], bits[0], bits[1])
                    second = mux(e[1:], bits[0], bits[1])
                    total = first * c0 + second * c1 + jnp.where(own2[c], beside, 0.0) + jnp.where(own[c], along, 0.0)
                    row = PAD + 2 * (2 * u + h) + c
                    out_ref[pl.ds(i * (4 * S) + row, 1), :] = jnp.sum(total, axis=0, keepdims=True)
        return carry

    lax.fori_loop(0, OWNERS // S, step, 0)


def merge_kernel(d_ref, r1_ref, r2_ref, out_ref, tile_ref, sem):
    sub = lax.broadcasted_iota(i32, (8, 128), 0)
    top, mid = sub < 2, sub < 4
    copies = []
    for k in range(MERGES):
        for src in range(k * OWNERS // MERGES, (k + 1) * OWNERS // MERGES):
            for h in range(2):
                slot = 2 * src + h
                w = r1_ref[src * HEAD_ROWS + 2 * h:src * HEAD_ROWS + 2 * h + 8, :]
                at = src * BODY_ROWS + BODY * h - 2
                u = r2_ref[at:at + 8, :] if slot else pltpu.roll(r2_ref[0:8, :], 2, 0)
                d = d_ref[PAD + 2 * slot - 2:PAD + 2 * slot + 6, :]
                tile_ref[:, slot * 128:slot * 128 + 128] = jnp.where(top, w, jnp.where(mid, u + d, u))
        lanes = pl.ds(k * (tile_ref.shape[1] // MERGES), tile_ref.shape[1] // MERGES)
        copies.append(pltpu.make_async_copy(tile_ref.at[:, lanes], out_ref.at[:, lanes], sem.at[k]))
        copies[-1].start()
    for copy in copies:
        copy.wait()


def shape(*dims, dt=f32):
    return jax.ShapeDtypeStruct(dims, dt)


def held(*dims, dt=f32):
    return pltpu.VMEM(dims, dt)


def near_memory(x):
    return pltpu.with_memory_space_constraint(x, pltpu.VMEM)


def scratch(width, size):
    rows = 128 * width + 16
    return [pltpu.VMEM((16384 // size, rows, 256), f32), pltpu.VMEM((rows, size), bf16), pltpu.VMEM((256, size), bf16)]


def head(particles, key, a, b, velocity):
    n = particles.shape[1]
    return pl.pallas_call(
        head_kernel,
        out_shape=(held(OWNERS * HEAD_ROWS, 128), held(1, n), held(128, 128)),
        in_specs=[pl.BlockSpec(memory_space=pl.ANY)] + [VMEM] * 3 + [pl.BlockSpec(memory_space=pl.ANY)],
        out_specs=(VMEM,) * 3,
        scratch_shapes=scratch(HEAD, n)
        + [pltpu.VMEM((256, 256), bf16), pltpu.VMEM((RB // 2, 256), bf16), pltpu.VMEM((2, 256, 128), f32), pltpu.VMEM((8, n), f32), pltpu.SemaphoreType.DMA((2,))],
        name="head",
    )(particles, key, a, b, velocity)


def body(particles, key, rank, count, velocity):
    return pl.pallas_call(
        body_kernel,
        out_shape=(held(OWNERS * BODY_ROWS, 128), held(512, 256, dt=bf16)),
        in_specs=[VMEM] * 5,
        out_specs=(VMEM,) * 2,
        scratch_shapes=scratch(BODY, particles.shape[1] // 2),
        name="body",
    )(particles, key, near_memory(rank), near_memory(count), velocity)


def interp(arrived, fields):
    return pl.pallas_call(
        interp_kernel,
        out_shape=(held(PAD + 4 * OWNERS + 8, 128), shape(2 * OWNERS, 128, dt=i32)),
        in_specs=[VMEM] * 2,
        out_specs=(VMEM,) * 2,
        name="interp",
    )(arrived, near_memory(fields))


def merge(moved, head_arrived, body_arrived):
    n = OWNERS * 256
    return pl.pallas_call(
        merge_kernel,
        out_shape=shape(8, n),
        in_specs=[VMEM] * 3,
        out_specs=pl.BlockSpec(memory_space=pl.ANY),
        scratch_shapes=[pltpu.VMEM((8, n), f32), pltpu.SemaphoreType.DMA((MERGES,))],
        name="merge",
    )(near_memory(moved), head_arrived, body_arrived)


def exchange(buckets, rows):
    out = lax.all_to_all(buckets.reshape(OWNERS, rows, 1, 128), ALL, 0, 0, tiled=True)
    return near_memory(out.reshape(OWNERS * rows, 128))


def shards(particles, dest_key, cell_a, cell_b, velocity):
    key, a, b = [v.reshape(1, -1) for v in (dest_key, cell_a, cell_b)]
    first, rank, count = head(particles, key, a, b, velocity)
    arrived = exchange(first, HEAD_ROWS)
    second, fields = body(particles, key, rank, count, velocity)
    rest = exchange(second, BODY_ROWS)
    moved, cell = interp(arrived, fields)
    return merge(moved, arrived, rest), cell.reshape(-1)


def solution(mesh):
    split_mesh = Mesh(mesh.devices.reshape(mesh.shape["gx"], 4, 4, mesh.shape["gz"]), ALL)
    in_specs = (P(None, ALL), P(ALL), P(ALL), P(ALL), P(None, "gx", WIDE))
    out_specs = (P(None, ALL), P(ALL))
    return jax.shard_map(shards, mesh=split_mesh, in_specs=in_specs, out_specs=out_specs, check_vma=False)
```
